32 devices in a mesh: section: 2 (over core), row: 4 (over y, x), col: 4 (over z).
Axes of the slice: x: 2, y: 2, z: 4, core: 2. Of those that a mesh axis runs over, the one named last changes fastest.
Arguments:
- section_inputs: bfloat16 [2, 2, 48, 4096], P('section', None, 'col', 'row'), may hold values from -6 to 6
- out_grad: bfloat16 [2, 48, 4096], P(None, 'col', 'row'), may hold values from -6 to 6
- gate_weight: bfloat16 [2, 4096, 14336], P('section', 'row', 'col'), may hold values from -0.09375 to 0.09375
- up_weight: bfloat16 [2, 4096, 14336], P('section', 'row', 'col'), may hold values from -0.09375 to 0.09375
- down_weight: bfloat16 [2, 14336, 4096], P('section', 'col', 'row'), may hold values from -0.046875 to 0.046875
Outputs:
- input_grads: bfloat16 [2, 2, 48, 4096], P('section', None, 'col', 'row')
- grad_gate: float32 [2, 4096, 14336], P('section', 'row', 'col')
- grad_up: float32 [2, 4096, 14336], P('section', 'row', 'col')
- grad_down: float32 [2, 14336, 4096], P('section', 'col', 'row')
The draws below stay inside these ranges and needn't reach their ends.
All inputs are finite; a program needn't handle non-finite values.
Results may differ from the reference program's by a relative error of at most 0.025.
Values may be sent and summed in bfloat16 or wider, within the bound.
A program may use at most 192 MiB of HBM per device.

```python
import jax
import jax.numpy as jnp

D = 4096
FF = 14336
MICRO = 2
SECTIONS = 2
TOKENS = 48
N_ROW = 4


def level_of(own_key, shape, pieces, low, top_value):
    gain, own = 1.0, jax.random.fold_in(own_key, 6)
    for position, shards_of in pieces:
        steps = jnp.exp(jax.random.uniform(jax.random.fold_in(own, position), (shards_of,), jnp.float32, low / len(pieces), top_value / len(pieces)))
        gain = gain * jnp.repeat(steps, shape[position] // shards_of).reshape([-1 if axis == position else 1 for axis in range(len(shape))])
    return gain


def gaussian(own_key, extent, scale, most, cuts=(), dtype=jnp.bfloat16):
    result = scale * jax.random.normal(own_key, extent, jnp.float32)
    if cuts:
        result = result * level_of(own_key, extent, cuts, -0.22, 0.18)
    return jnp.clip(result, -most, most).astype(dtype)


def setup_inputs(seed: int = 0) -> dict:
    arg_keys = jax.random.split(jax.random.key(seed), 6)
    section_inputs = gaussian(arg_keys[0], (SECTIONS, MICRO, TOKENS, D), 1.0, 6.0, ((0, 2), (2, 4), (3, 4)))
    out_grad = gaussian(arg_keys[1], (MICRO, TOKENS, D), 1.0, 6.0, ((1, 4), (2, 4)))
    gate_weight = gaussian(arg_keys[2], (SECTIONS, D, FF), D ** -0.5, 0.09375, ((0, 2), (1, 4), (2, 4)))
    up_weight = gaussian(arg_keys[3], (SECTIONS, D, FF), D ** -0.5, 0.09375, ((0, 2), (1, 4), (2, 4)))
    down_weight = gaussian(arg_keys[4], (SECTIONS, FF, D), FF ** -0.5, 0.046875, ((0, 2), (1, 4), (2, 4)))
    return dict(section_inputs=section_inputs, out_grad=out_grad, gate_weight=gate_weight, up_weight=up_weight, down_weight=down_weight)


def blocked_sum(left, right):
    width = D // N_ROW
    total = jnp.zeros((left.shape[0], right.shape[1]), jnp.float32)
    for block in range(N_ROW):
        piece = jnp.dot(left[:, block * width:(block + 1) * width], right[block * width:(block + 1) * width],
                        preferred_element_type=jnp.float32).astype(jnp.bfloat16)
        total = total + piece.astype(jnp.float32)
    return total


def layer_backward(x_rows, dy_rows, w_gate, w_up, w_down):
    gate_sum = blocked_sum(x_rows, w_gate)
    up_sum = blocked_sum(x_rows, w_up)
    sigmoid_gate = jax.nn.sigmoid(gate_sum)
    activated = gate_sum * sigmoid_gate
    slope = sigmoid_gate * (1.0 + gate_sum * (1.0 - sigmoid_gate))
    hidden = (activated * up_sum).astype(jnp.bfloat16)
    hidden_grad = blocked_sum(dy_rows, w_down.T)
    gate_grad = (hidden_grad * up_sum * slope).astype(jnp.bfloat16)
    up_grad = (hidden_grad * activated).astype(jnp.bfloat16)
    branch = jnp.dot(gate_grad, w_gate.T, preferred_element_type=jnp.float32)
    branch = branch + jnp.dot(up_grad, w_up.T, preferred_element_type=jnp.float32)
    input_grad = (dy_rows.astype(jnp.float32) + branch).astype(jnp.bfloat16)
    gate_update = jnp.dot(x_rows.T, gate_grad, preferred_element_type=jnp.float32)
    up_update = jnp.dot(x_rows.T, up_grad, preferred_element_type=jnp.float32)
    down_update = jnp.dot(hidden.T, dy_rows, preferred_element_type=jnp.float32)
    return input_grad, gate_update, up_update, down_update


def reference(section_inputs, out_grad, gate_weight, up_weight, down_weight):
    carried = [out_grad[micro_index] for micro_index in range(MICRO)]
    input_list = []
    gate_list = []
    up_list = []
    down_list = []
    for section_number in reversed(range(SECTIONS)):
        gate_total = jnp.zeros((D, FF), jnp.float32)
        up_total = jnp.zeros((D, FF), jnp.float32)
        down_total = jnp.zeros((FF, D), jnp.float32)
        produced = []
        for micro_index in range(MICRO):
            input_grad, gate_update, up_update, down_update = layer_backward(
                section_inputs[section_number, micro_index], carried[micro_index],
                gate_weight[section_number], up_weight[section_number], down_weight[section_number])
            produced.append(input_grad)
            gate_total = gate_total + gate_update
            up_total = up_total + up_update
            down_total = down_total + down_update
        carried = produced
        input_list.insert(0, jnp.stack(produced))
        gate_list.insert(0, gate_total)
        up_list.insert(0, up_total)
        down_list.insert(0, down_total)
    return jnp.stack(input_list), jnp.stack(gate_list), jnp.stack(up_list), jnp.stack(down_list)
```

```python
import jax
import jax.numpy as jnp
from jax import lax
from jax.experimental import pallas as pl
from jax.experimental.pallas import tpu as pltpu
from jax.sharding import PartitionSpec as P

CONTRACT_ROWS = (((0,), (0,)), ((), ()))
CONTRACT_COLS = (((1,), (1,)), ((), ()))


def passed_along(block, axis, distance):
    devices = range(lax.axis_size(axis))
    route = [(i - distance, i) for i in devices if i - distance in devices]
    return lax.ppermute(block, axis, route)


def spread_panel(panel):
    return lax.all_gather(panel, "col", axis=0, tiled=True)


def row_partials(make_terms, keep_rows):
    return lax.psum_scatter(
        make_terms(jnp.int32(0), keep_rows * lax.axis_size("row")).astype(jnp.bfloat16),
        "row",
        scatter_dimension=0,
        tiled=True,
    ).astype(jnp.float32)


def layer_backward(x_local, dy_local, w_both, w_down):
    hidden_width = w_down.shape[0]
    x_whole = spread_panel(x_local)
    dy_whole = spread_panel(dy_local)
    keep_rows = x_whole.shape[0] // lax.axis_size("row")

    def forward_terms(first_row, row_count):
        return jnp.dot(x_whole, w_both, preferred_element_type=jnp.float32)

    def backward_terms(first_row, row_count):
        return lax.dot_general(dy_whole, w_down, CONTRACT_COLS, preferred_element_type=jnp.float32)

    both_sums = row_partials(forward_terms, keep_rows)
    hidden_grad = row_partials(backward_terms, keep_rows)
    gate_sum = both_sums[:, :hidden_width]
    up_sum = both_sums[:, hidden_width:]
    sigmoid_gate = jax.nn.sigmoid(gate_sum)
    activated = gate_sum * sigmoid_gate
    slope = sigmoid_gate * (1.0 + gate_sum * (1.0 - sigmoid_gate))
    hidden = (activated * up_sum).astype(jnp.bfloat16)
    gate_grad = (hidden_grad * up_sum * slope).astype(jnp.bfloat16)
    up_grad = (hidden_grad * activated).astype(jnp.bfloat16)
    packed = jnp.concatenate([hidden, gate_grad, up_grad], axis=1)
    gathered = lax.all_gather(packed, "row", axis=0, tiled=True)
    hidden_whole = gathered[:, :hidden_width]
    both_grads = gathered[:, hidden_width:]
    branch_sum = lax.psum_scatter(
        lax.dot_general(
            both_grads, w_both, CONTRACT_COLS, preferred_element_type=jnp.float32
        ).astype(jnp.bfloat16),
        "col",
        scatter_dimension=0,
        tiled=True,
    ).astype(jnp.float32)
    input_grad = (dy_local.astype(jnp.float32) + branch_sum).astype(jnp.bfloat16)
    down_update = lax.dot_general(
        hidden_whole, dy_whole, CONTRACT_ROWS, preferred_element_type=jnp.float32
    )
    both_update = lax.dot_general(
        x_whole, both_grads, CONTRACT_ROWS, preferred_element_type=jnp.float32
    )
    return (input_grad, both_update, down_update)


def shards(section_inputs, out_grad, gate_weight, up_weight, down_weight):
    section_id = lax.axis_index("section")
    last_section = lax.axis_size("section") - 1
    is_last = section_id == last_section
    panels = section_inputs[0]
    w_both = jnp.concatenate([gate_weight[0], up_weight[0]], axis=1)
    w_down = down_weight[0]
    hidden_width = w_down.shape[0]
    micro_count = panels.shape[0]
    both_total = jnp.zeros(w_both.shape, jnp.float32)
    down_total = jnp.zeros(w_down.shape, jnp.float32)
    merged_shape = (micro_count * panels.shape[1], panels.shape[2])
    x_local = panels.reshape(merged_shape)
    top_grads = out_grad.reshape(merged_shape)
    received = jnp.zeros(merged_shape, jnp.bfloat16)
    merged_results = received
    for step_index in range(last_section + 1):
        is_active = section_id == last_section - step_index
        dy_local = jnp.where(is_last, top_grads, received)
        input_grad, both_update, down_update = layer_backward(x_local, dy_local, w_both, w_down)
        merged_results = jnp.where(is_active, input_grad, merged_results)
        both_total = both_total + jnp.where(is_active, both_update, 0.0)
        down_total = down_total + jnp.where(is_active, down_update, 0.0)
        if step_index < last_section:
            received = passed_along(input_grad, "section", -1)
    results = merged_results.reshape(panels.shape)
    return (
        results[None],
        both_total[:, :hidden_width][None],
        both_total[:, hidden_width:][None],
        down_total[None],
    )


ORDER = pl.DeviceIdType.MESH


def remote(src, dst, send_sem, recv_sem, target):
    return pltpu.make_async_remote_copy(
        src_ref=src, dst_ref=dst, send_sem=send_sem, recv_sem=recv_sem, device_id=target, device_id_type=ORDER
    )


def relay_kernel(
    x_ref, top_ref, gate_ref, up_ref, down_ref,
    grad_out, x_out, dy_out, packed_out,
    w_gate, w_up, w_down, x_slots, dy_slots, x_whole, dy_whole, stage, part_send, part_recv, spread, gate_sum, up_sum, terms,
    branch, branch_send, branch_recv, result,
    w_sem, in_sem, x_send_sem, x_recv_sem, dy_send_sem, dy_recv_sem, part_send_sem, part_recv_sem,
    spread_send_sem, spread_recv_sem, onward_send_sem, onward_recv_sem, branch_send_sem, branch_recv_sem, out_sem, last_sem,
    go_sem,
):
    section = lax.axis_index("section")
    row = lax.axis_index("row")
    col = lax.axis_index("col")
    rows, width = part_send.shape[2], part_send.shape[3]
    local, micro = x_slots.shape[1:3]
    span = rows // 2
    group = local * micro
    block = x_slots.shape[3] // 2
    is_top = section == 1
    is_bottom = section == 0

    def row_peer(d):
        hi, lo = row // 2, row % 2
        return ((hi + d // 2) % 2) * 2 + (lo + d % 2) % 2

    def ahead(d):
        return (col + d) % 4

    def behind(d):
        return (col + 4 - d) % 4

    def half(h):
        return pl.ds(h * span, span)

    def block_of(c):
        return pl.ds(pl.multiple_of(c * block, block), block)

    def weight_copy(a, d):
        cols = pl.ds(pl.multiple_of(row_peer(d) * width, width), width)
        if a == 2:
            return pltpu.make_async_copy(down_ref.at[cols, :], w_down.at[d], w_sem.at[2, d])
        source, target = ((gate_ref, w_gate), (up_ref, w_up))[a]
        return pltpu.make_async_copy(source.at[:, cols], target.at[d], w_sem.at[a, d])

    def x_copy(d):
        return remote(x_slots.at[0], x_slots.at[d], x_send_sem.at[d], x_recv_sem.at[d], (section, row, ahead(d)))

    def dy_copy(d, c):
        return remote(
            dy_slots.at[c, 0], dy_slots.at[c, d], dy_send_sem.at[d, c], dy_recv_sem.at[d, c], (section, row, ahead(d))
        )

    def pass_copy(d, c):
        return remote(
            result.at[c], dy_slots.at[c, d], dy_send_sem.at[d, c], dy_recv_sem.at[d, c], (0, row, ahead(d))
        )

    def part_copy(a, d, h):
        place = (a, d, half(h), slice(None))
        via = (d - 2 * (d // 3), d - d // 3, d)[a]
        return remote(
            part_send.at[place], part_recv.at[place],
            part_send_sem.at[a, d, h], part_recv_sem.at[a, d, h], (section, row_peer(via), col),
        )

    def relay_sum(a, h):
        middle = 2 - a
        part_copy(a, 3, h).wait_recv()
        total = part_send[a, middle, half(h), :].astype(jnp.float32) + part_recv[a, 3, half(h), :].astype(jnp.float32)
        part_send[a, middle, half(h), :] = total.astype(jnp.bfloat16)
        part_copy(a, middle, h).start()

    def spread_copy(a, d, h):
        return remote(
            spread.at[a, 0, half(h), :], spread.at[a, d, half(h), :],
            spread_send_sem.at[a, d, h], spread_recv_sem.at[a, d, h], (section, row_peer(d), col),
        )

    def onward_copy(a, h):
        d = (1 + h, 1, 2)[a]
        return remote(
            spread.at[a, d, half(h), :], spread.at[a, 3, half(h), :],
            onward_send_sem.at[a, h], onward_recv_sem.at[a, h], (section, row_peer(3 - d), col),
        )

    def spread_grads(h):
        for a, d in ((1, 1), (2, 2), (2, 1), (1, 2)):
            spread_copy(a, d, h).start()

    def relay_grads(h):
        for a in (1, 2):
            spread_copy(a, a, h).wait_recv()
            onward_copy(a, h).start()

    def spread_hidden():
        for h, d in ((0, 1), (1, 2), (1, 1), (0, 2)):
            spread_copy(0, d, h).start()

    def relay_hidden():
        for h in range(2):
            spread_copy(0, 1 + h, h).wait_recv()
            onward_copy(0, h).start()

    def branch_copy(d, c):
        return remote(
            branch_send.at[c, d], branch_recv.at[c, d], branch_send_sem.at[d, c], branch_recv_sem.at[d, c],
            (section, row, behind(d)),
        )

    def store_copy(a, d):
        cols = pl.ds(pl.multiple_of(row_peer(d) * width, width), width)
        return pltpu.make_async_copy(spread.at[a, d], packed_out.at[a, :, cols], out_sem.at[a, d])

    def last_copy(which, c):
        source, target = (
            (x_whole.at[:, block_of(c)], x_out.at[:, block_of(c)]),
            (dy_whole.at[c], dy_out.at[:, block_of(c)]),
            (result.at[c], grad_out.at[:, :, block_of(c)]),
        )[which]
        return pltpu.make_async_copy(source, target, last_sem.at[which, c])

    def merge(slots, arrive):
        for d in range(4):
            arrive(d)
            for t in range(local):
                first = d * group + t * micro
                stage[first:first + micro, :slots.shape[3]] = slots[d, t].astype(jnp.float32)

    def merge_dy(c, arrive):
        merge(dy_slots.at[c], arrive)
        dy_whole[c] = stage[:, :block].astype(jnp.bfloat16)
        last_copy(1, c).start()

    x_load = pltpu.make_async_copy(x_ref, x_slots.at[0], in_sem.at[0])

    def top_load(c):
        return pltpu.make_async_copy(top_ref.at[:, :, block_of(c)], dy_slots.at[c, 0], in_sem.at[1 + c])

    x_load.start()

    @pl.when(is_top)
    def _():
        for c in range(2):
            top_load(c).start()

    barrier = pltpu.get_barrier_semaphore()
    greeted = [(section, row, ahead(d)) for d in (1, 2, 3)]
    greeted += [(section, row_peer(d), col) for d in (1, 2, 3)]
    greeted += [(1 - section, row, ahead(d)) for d in range(4)]
    for device in greeted:
        pl.semaphore_signal(barrier, inc=1, device_id=device, device_id_type=ORDER)
    x_load.wait()

    @pl.when(is_top)
    def _():
        for c in range(2):
            top_load(c).wait()

    for d in (3, 2, 1, 0):
        weight_copy(0, d).start()
        weight_copy(1, d).start()
    for d in (3, 2, 1, 0):
        weight_copy(2, d).start()

    pl.semaphore_wait(barrier, len(greeted))

    def partner_go(which):
        pl.semaphore_signal(
            go_sem.at[which], inc=1, device_id=(1 - section, row, col), device_id_type=ORDER
        )

    @pl.when(is_bottom)
    def _():
        pl.semaphore_wait(go_sem.at[0], 1)

    for d in (2, 1, 3):
        x_copy(d).start()

    @pl.when(is_top)
    def _():
        for c in range(2):
            for d in (2, 1, 3):
                dy_copy(d, c).start()

    def x_arrive(d):
        if d:
            x_copy(d).wait_recv()

    merge(x_slots, x_arrive)

    @pl.when(is_top)
    def _():
        partner_go(0)

    x_whole[...] = stage[...].astype(jnp.bfloat16)
    for c in range(2):
        last_copy(0, c).start()

    def forward_step(i, carry):
        d = 3 - i
        weight_copy(0, d).wait()
        weight_copy(1, d).wait()
        for a, weight in enumerate((w_gate, w_up)):
            part_send[a, d] = jnp.dot(
                x_whole[...], weight[d], preferred_element_type=jnp.float32
            ).astype(jnp.bfloat16)

            @pl.when(jnp.logical_and(is_top, (d % 2 == 1, d >= 2)[a]))
            def _():
                for h in range(2):
                    part_copy(a, d, h).start()
        return carry

    lax.fori_loop(0, 4, forward_step, 0)

    def summed(a, where):
        total = part_send[a, 0, where, :].astype(jnp.float32)
        for d in range(1, 4 if a == 2 else 3):
            total = total + part_recv[a, d, where, :].astype(jnp.float32)
        return total

    def rows_of(i):
        return pl.ds(pl.multiple_of(i * 16, 16), 16)

    def hidden_step(i, carry):
        where = rows_of(i)
        gate, up = summed(0, where), summed(1, where)
        gate_sum[where, :] = gate
        up_sum[where, :] = up
        spread[0, 0, where, :] = (gate * jax.nn.sigmoid(gate) * up).astype(jnp.bfloat16)
        return carry

    def grad_step(i, carry):
        where = rows_of(i)
        hidden_grad = summed(2, where)
        gate, up = gate_sum[where, :], up_sum[where, :]
        sigmoid_gate = jax.nn.sigmoid(gate)
        slope = sigmoid_gate * (1.0 + gate * (1.0 - sigmoid_gate))
        spread[1, 0, where, :] = (hidden_grad * up * slope).astype(jnp.bfloat16)
        spread[2, 0, where, :] = (hidden_grad * (gate * sigmoid_gate)).astype(jnp.bfloat16)
        return carry

    steps = span // 16

    def hidden_rows(h):
        for a in range(2):
            for d in (1, 2):
                part_copy(a, d, h).wait_recv()
        lax.fori_loop(h * steps, (h + 1) * steps, hidden_step, 0)

    def grad_rows(h):
        for d in (1, 2, 3):
            part_copy(2, d, h).wait_recv()
        lax.fori_loop(h * steps, (h + 1) * steps, grad_step, 0)
        spread_grads(h)

    @pl.when(is_bottom)
    def _():
        pl.semaphore_wait(go_sem.at[1], 1)
        for a, d in ((0, 3), (1, 3), (0, 1), (1, 2)):
            for h in range(2):
                part_copy(a, d, h).start()

    for a in range(2):
        relay_sum(a, 0)

    @pl.when(is_bottom)
    def _():
        for a in range(2):
            relay_sum(a, 1)
        for h in range(2):
            hidden_rows(h)
        spread_hidden()

    def merge_block(c):
        @pl.when(is_top)
        def _():
            merge_dy(c, lambda d: dy_copy(d, c).wait_recv() if d else None)

        @pl.when(is_bottom)
        def _():
            merge_dy(c, lambda d: pass_copy(d, c).wait_recv())

    def grad_terms_step(k, carry):
        c = section * (k % 2) + (1 - section) * (k // 4)
        d = 3 - section * (k // 2) - (1 - section) * (k % 4)

        @pl.when(k == 0)
        def _():
            merge_block(0)

        @pl.when(k == 4 - 3 * section)
        def _():
            merge_block(1)

        @pl.when(jnp.logical_and(is_top, k == 4))
        def _():
            for a in range(2):
                relay_sum(a, 1)

        @pl.when(c == 0)
        def _():
            weight_copy(2, d).wait()

        term = lax.dot_general(
            dy_whole[c], w_down[d, :, block_of(c)], CONTRACT_COLS, preferred_element_type=jnp.float32
        )

        @pl.when(c == 0)
        def _():
            terms[d] = term

        @pl.when(c == 1)
        def _():
            part_send[2, d] = (terms[d] + term).astype(jnp.bfloat16)

            @pl.when(d > 0)
            def _():
                part_copy(2, d, 0).start()
        return carry

    lax.fori_loop(0, 8, grad_terms_step, 0)
    for d in (3, 2, 1):
        part_copy(2, d, 1).start()

    @pl.when(is_top)
    def _():
        for h in range(2):
            hidden_rows(h)

    @pl.when(is_bottom)
    def _():
        relay_hidden()

    for h in range(2):
        grad_rows(h)

    def send_branch(c):
        for d in (2, 3, 1):
            first = d * group
            branch_send[c, d] = branch[c, first:first + group, :].astype(jnp.bfloat16)
            branch_copy(d, c).start()

    def branch_step(k, carry):
        d = k // 2
        c = k % 2

        @pl.when(k == 2)
        def _():
            for h in range(2):
                relay_grads(h)

            @pl.when(is_top)
            def _():
                partner_go(1)
                spread_hidden()

            for h in range(2):
                spread_copy(2, 1, h).wait_recv()

        @pl.when(k == 4)
        def _():
            for h in range(2):
                spread_copy(1, 2, h).wait_recv()

        @pl.when(k == 6)
        def _():
            for h in range(2):
                for a in (1, 2):
                    onward_copy(a, h).wait_recv()

        @pl.when(k == 7)
        def _():
            send_branch(0)

        term = lax.dot_general(
            spread[1, d], w_gate[d, block_of(c), :], CONTRACT_COLS, preferred_element_type=jnp.float32
        ) + lax.dot_general(
            spread[2, d], w_up[d, block_of(c), :], CONTRACT_COLS, preferred_element_type=jnp.float32
        )

        @pl.when(d == 0)
        def _():
            branch[c] = term

        @pl.when(d > 0)
        def _():
            branch[c] += term
        return carry

    lax.fori_loop(0, 8, branch_step, 0)
    send_branch(1)
    for a in (1, 2):
        for d in range(4):
            store_copy(a, d).start()

    for c in range(2):
        total = dy_whole[c, :group, :].astype(jnp.float32) + branch[c, :group, :]
        for d in (1, 2, 3):
            branch_copy(d, c).wait_recv()
            total = total + branch_recv[c, d].astype(jnp.float32)
        stage[:group, :block] = total
        for t in range(local):
            result[c, t] = stage[t * micro:(t + 1) * micro, :block].astype(jnp.bfloat16)

        @pl.when(is_top)
        def _():
            for d in (2, 3, 1, 0):
                pass_copy(d, c).start()

        last_copy(2, c).start()

    @pl.when(is_top)
    def _():
        relay_hidden()

    for h in range(2):
        spread_copy(0, 2 - h, h).wait_recv()
        onward_copy(0, h).wait_recv()
    for d in range(4):
        store_copy(0, d).start()
    for d in (1, 2, 3):
        x_copy(d).wait_send()
        for h in range(2):
            branch_copy(d, h).wait_send()
            for a in range(3):
                part_copy(a, d, h).wait_send()
    for h in range(2):
        for a in range(3):
            for d in (1, 2):
                spread_copy(a, d, h).wait_send()
            onward_copy(a, h).wait_send()

    @pl.when(is_top)
    def _():
        for h in range(2):
            for d in (1, 2, 3):
                dy_copy(d, h).wait_send()
            for d in range(4):
                pass_copy(d, h).wait_send()

    for a in range(3):
        for d in range(4):
            store_copy(a, d).wait()
    for which in range(3):
        for c in range(2):
            last_copy(which, c).wait()


def update_kernel(x_ref, dy_ref, packed_ref, gate_out, up_out, down_out):
    for left, right, out in (
        (x_ref[...], packed_ref[1], gate_out),
        (x_ref[...], packed_ref[2], up_out),
        (packed_ref[0], dy_ref[...], down_out),
    ):
        out[...] = lax.dot_general(left, right, CONTRACT_ROWS, preferred_element_type=jnp.float32)


def weight_updates(x_whole, dy_whole, packed):
    rows, width = x_whole.shape
    hidden_width = packed.shape[2]
    tile = next(t for t in (512, 256, 128) if hidden_width % t == 0)
    f32 = jnp.float32
    whole = pl.BlockSpec((rows, width), lambda j: (0, 0))
    wide = pl.BlockSpec((width, tile), lambda j: (0, j))
    return pl.pallas_call(
        update_kernel,
        grid=(hidden_width // tile,),
        out_shape=(
            jax.ShapeDtypeStruct((width, hidden_width), f32),
            jax.ShapeDtypeStruct((width, hidden_width), f32),
            jax.ShapeDtypeStruct((hidden_width, width), f32),
        ),
        in_specs=[whole, whole, pl.BlockSpec((3, rows, tile), lambda j: (0, 0, j))],
        out_specs=(wide, wide, pl.BlockSpec((tile, width), lambda j: (j, 0))),
        compiler_params=pltpu.CompilerParams(vmem_limit_bytes=60 * 2**20),
    )(x_whole, dy_whole, packed)


def fast_shards(section_inputs, out_grad, gate_weight, up_weight, down_weight):
    panels = section_inputs[0]
    micro, local, width = panels.shape
    group = micro * local
    held = (local, micro, width)
    rows = group * lax.axis_size("col")
    hidden_width = gate_weight.shape[2]
    piece = hidden_width // lax.axis_size("row")
    hbm = pl.BlockSpec(memory_space=pltpu.HBM)
    bf16, f32 = jnp.bfloat16, jnp.float32
    dma = pltpu.SemaphoreType.DMA
    block = width // 2
    grad, x_whole, dy_whole, packed = pl.pallas_call(
        relay_kernel,
        out_shape=(
            jax.ShapeDtypeStruct(held, bf16),
            jax.ShapeDtypeStruct((rows, width), bf16),
            jax.ShapeDtypeStruct((rows, width), bf16),
            jax.ShapeDtypeStruct((3, rows, hidden_width), bf16),
        ),
        in_specs=[hbm] * 5,
        out_specs=(hbm,) * 4,
        scratch_shapes=[
            pltpu.VMEM((4, width, piece), bf16),
            pltpu.VMEM((4, width, piece), bf16),
            pltpu.VMEM((4, piece, width), bf16),
            pltpu.VMEM((4, *held), bf16),
            pltpu.VMEM((2, 4, local, micro, block), bf16),
            pltpu.VMEM((rows, width), bf16),
            pltpu.VMEM((2, rows, block), bf16),
            pltpu.VMEM((rows, width), f32),
            pltpu.VMEM((3, 4, rows, piece), bf16),
            pltpu.VMEM((3, 4, rows, piece), bf16),
            pltpu.VMEM((3, 4, rows, piece), bf16),
            pltpu.VMEM((rows, piece), f32),
            pltpu.VMEM((rows, piece), f32),
            pltpu.VMEM((4, rows, piece), f32),
            pltpu.VMEM((2, rows, block), f32),
            pltpu.VMEM((2, 4, group, block), bf16),
            pltpu.VMEM((2, 4, group, block), bf16),
            pltpu.VMEM((2, local, micro, block), bf16),
            dma((3, 4)), dma((3,)), dma((4,)), dma((4,)), dma((4, 2)), dma((4, 2)), dma((3, 4, 2)), dma((3, 4, 2)),
            dma((3, 4, 2)), dma((3, 4, 2)), dma((3, 2)), dma((3, 2)), dma((4, 2)), dma((4, 2)), dma((3, 4)), dma((3, 2)),
            pltpu.SemaphoreType.REGULAR((2,)),
        ],
        compiler_params=pltpu.CompilerParams(collective_id=0, has_side_effects=True, vmem_limit_bytes=56 * 2**20),
    )(
        panels.transpose(1, 0, 2), out_grad.transpose(1, 0, 2),
        gate_weight[0], up_weight[0], down_weight[0],
    )
    grads = weight_updates(x_whole, dy_whole, packed)
    grad = grad.transpose(1, 0, 2)
    return (grad[None], *(g[None] for g in grads))


def fits_kernel(mesh, gate_weight, section_inputs):
    sizes = mesh.shape
    if (sizes["section"], sizes["row"], sizes["col"]) != (2, 4, 4):
        return False
    piece = gate_weight.shape[2] // (sizes["row"] * sizes["col"])
    local = section_inputs.shape[1] * section_inputs.shape[2] // sizes["col"]
    return piece % 128 == 0 and local % 8 == 0 and (local * sizes["col"]) % 32 == 0


def solution(mesh):
    specs = dict(
        mesh=mesh,
        in_specs=(
            P("section", None, "col", "row"),
            P(None, "col", "row"),
            P("section", "row", "col"),
            P("section", "row", "col"),
            P("section", "col", "row"),
        ),
        out_specs=(
            P("section", None, "col", "row"),
            P("section", "row", "col"),
            P("section", "row", "col"),
            P("section", "col", "row"),
        ),
        check_vma=False,
    )

    def run(section_inputs, out_grad, gate_weight, up_weight, down_weight):
        body = fast_shards if fits_kernel(mesh, gate_weight, section_inputs) else shards
        return jax.shard_map(body, **specs)(section_inputs, out_grad, gate_weight, up_weight, down_weight)

    return run
```

```python
import jax
import jax.numpy as jnp
from jax import lax
from jax.experimental import pallas as pl
from jax.experimental.pallas import tpu as pltpu
from jax.sharding import PartitionSpec as P

CONTRACT_ROWS = (((0,), (0,)), ((), ()))
CONTRACT_COLS = (((1,), (1,)), ((), ()))


def passed_along(block, axis, distance):
    devices = range(lax.axis_size(axis))
    route = [(i - distance, i) for i in devices if i - distance in devices]
    return lax.ppermute(block, axis, route)


def spread_panel(panel):
    return lax.all_gather(panel, "col", axis=0, tiled=True)


def row_partials(make_terms, keep_rows):
    return lax.psum_scatter(
        make_terms(jnp.int32(0), keep_rows * lax.axis_size("row")).astype(jnp.bfloat16),
        "row",
        scatter_dimension=0,
        tiled=True,
    ).astype(jnp.float32)


def layer_backward(x_local, dy_local, w_both, w_down):
    hidden_width = w_down.shape[0]
    x_whole = spread_panel(x_local)
    dy_whole = spread_panel(dy_local)
    keep_rows = x_whole.shape[0] // lax.axis_size("row")

    def forward_terms(first_row, row_count):
        return jnp.dot(x_whole, w_both, preferred_element_type=jnp.float32)

    def backward_terms(first_row, row_count):
        return lax.dot_general(dy_whole, w_down, CONTRACT_COLS, preferred_element_type=jnp.float32)

    both_sums = row_partials(forward_terms, keep_rows)
    hidden_grad = row_partials(backward_terms, keep_rows)
    gate_sum = both_sums[:, :hidden_width]
    up_sum = both_sums[:, hidden_width:]
    sigmoid_gate = jax.nn.sigmoid(gate_sum)
    activated = gate_sum * sigmoid_gate
    slope = sigmoid_gate * (1.0 + gate_sum * (1.0 - sigmoid_gate))
    hidden = (activated * up_sum).astype(jnp.bfloat16)
    gate_grad = (hidden_grad * up_sum * slope).astype(jnp.bfloat16)
    up_grad = (hidden_grad * activated).astype(jnp.bfloat16)
    packed = jnp.concatenate([hidden, gate_grad, up_grad], axis=1)
    gathered = lax.all_gather(packed, "row", axis=0, tiled=True)
    hidden_whole = gathered[:, :hidden_width]
    both_grads = gathered[:, hidden_width:]
    branch_sum = lax.psum_scatter(
        lax.dot_general(
            both_grads, w_both, CONTRACT_COLS, preferred_element_type=jnp.float32
        ).astype(jnp.bfloat16),
        "col",
        scatter_dimension=0,
        tiled=True,
    ).astype(jnp.float32)
    input_grad = (dy_local.astype(jnp.float32) + branch_sum).astype(jnp.bfloat16)
    down_update = lax.dot_general(
        hidden_whole, dy_whole, CONTRACT_ROWS, preferred_element_type=jnp.float32
    )
    both_update = lax.dot_general(
        x_whole, both_grads, CONTRACT_ROWS, preferred_element_type=jnp.float32
    )
    return (input_grad, both_update, down_update)


def shards(section_inputs, out_grad, gate_weight, up_weight, down_weight):
    section_id = lax.axis_index("section")
    last_section = lax.axis_size("section") - 1
    is_last = section_id == last_section
    panels = section_inputs[0]
    w_both = jnp.concatenate([gate_weight[0], up_weight[0]], axis=1)
    w_down = down_weight[0]
    hidden_width = w_down.shape[0]
    micro_count = panels.shape[0]
    both_total = jnp.zeros(w_both.shape, jnp.float32)
    down_total = jnp.zeros(w_down.shape, jnp.float32)
    merged_shape = (micro_count * panels.shape[1], panels.shape[2])
    x_local = panels.reshape(merged_shape)
    top_grads = out_grad.reshape(merged_shape)
    received = jnp.zeros(merged_shape, jnp.bfloat16)
    merged_results = received
    for step_index in range(last_section + 1):
        is_active = section_id == last_section - step_index
        dy_local = jnp.where(is_last, top_grads, received)
        input_grad, both_update, down_update = layer_backward(x_local, dy_local, w_both, w_down)
        merged_results = jnp.where(is_active, input_grad, merged_results)
        both_total = both_total + jnp.where(is_active, both_update, 0.0)
        down_total = down_total + jnp.where(is_active, down_update, 0.0)
        if step_index < last_section:
            received = passed_along(input_grad, "section", -1)
    results = merged_results.reshape(panels.shape)
    return (
        results[None],
        both_total[:, :hidden_width][None],
        both_total[:, hidden_width:][None],
        down_total[None],
    )


ORDER = pl.DeviceIdType.MESH


def remote(src, dst, send_sem, recv_sem, target):
    return pltpu.make_async_remote_copy(
        src_ref=src, dst_ref=dst, send_sem=send_sem, recv_sem=recv_sem, device_id=target, device_id_type=ORDER
    )


def relay_kernel(
    x_ref, top_ref, gate_ref, up_ref, down_ref,
    x_out, dy_out, packed_out, own_out, far_out_1, far_out_2, far_out_3,
    w_gate, w_up, w_down, turned, x_slots, dy_slots, x_whole, dy_whole, stage, part_send, part_recv, spread, gate_sum, up_sum, factors, middle,
    branch, branch_send, branch_recv, result,
    w_sem, in_sem, send_sem, x_recv_sem, dy_recv_sem, via_sem, pair_sem, last_part_sem,
    first_sem, second_sem, onward_sem, cross_sem, branch_recv_sem, out_sem, go_sem,
):
    section = lax.axis_index("section")
    row = lax.axis_index("row")
    col = lax.axis_index("col")
    rows, width = part_send.shape[2], part_send.shape[3]
    local, micro = x_slots.shape[1:3]
    span = rows // 2
    group = local * micro
    block = x_slots.shape[3] // 2
    is_top = section == 1
    is_bottom = section == 0

    def row_peer(d):
        hi, lo = row // 2, row % 2
        return ((hi + d // 2) % 2) * 2 + (lo + d % 2) % 2

    def ahead(d):
        return (col + d) % 4

    def behind(d):
        return (col + 4 - d) % 4

    def half(h):
        return pl.ds(h * span, span)

    def block_of(c):
        return pl.ds(pl.multiple_of(c * block, block), block)

    def piece_of(d):
        return pl.ds(pl.multiple_of(row_peer(d) * width, width), width)

    weights = ((gate_ref, w_gate), (up_ref, w_up), (down_ref, w_down))

    def weight_load(a):
        source, target = weights[a]
        size = target.shape[0] // 4
        for q in range(4):
            where = pl.ds(q * size, size)
            pltpu.make_async_copy(source.at[where, :], target.at[where, :], w_sem.at[a]).start()

    def weight_wait(a):
        source, target = weights[a]
        pltpu.make_async_copy(source, target, w_sem.at[a]).wait()

    def received(ref, sem):
        remote(ref, ref, send_sem.at[0], sem, (section, row, ahead(1))).wait_recv()

    def sent(ref, kind):
        remote(ref, ref, send_sem.at[kind], send_sem.at[kind], (section, row, ahead(1))).wait_send()

    def x_copy(d):
        return remote(x_slots.at[0], x_slots.at[d], send_sem.at[0], x_recv_sem.at[0], (section, row, ahead(d)))

    def dy_copy(d, c):
        return remote(
            dy_slots.at[c, 0], dy_slots.at[c, d], send_sem.at[1], dy_recv_sem.at[c], (section, row, ahead(d))
        )

    def pass_copy(d, c):
        return remote(result.at[c], dy_slots.at[c, d], send_sem.at[6], dy_recv_sem.at[c], (0, row, ahead(d)))

    def part_copy(a, d, h, via, sem):
        place = (a, d, half(h), slice(None))
        return remote(
            part_send.at[place], part_recv.at[place], send_sem.at[2], sem, (section, row_peer(via), col)
        )

    def via_copy(a, h):
        return part_copy(a, 3, h, 1 + a, via_sem.at[a, h])

    def pair_copy(a, d, h):
        return part_copy(a, d, h, d, pair_sem.at[h])

    def last_part_copy(d, h):
        return part_copy(2, d, h, d, last_part_sem.at[h])

    def relay_sum(a, h):
        middle = 2 - a
        via_copy(a, h).wait_recv()
        total = part_send[a, middle, half(h), :].astype(jnp.float32) + part_recv[a, 3, half(h), :].astype(jnp.float32)
        part_send[a, middle, half(h), :] = total.astype(jnp.bfloat16)
        pair_copy(a, middle, h).start()

    def spread_copy(a, d, h, sem):
        return remote(
            spread.at[a, 0, half(h), :], spread.at[a, d, half(h), :],
            send_sem.at[3], sem, (section, row_peer(d), col),
        )

    def first_copy(a, h):
        d = (1 + h, 1, 2)[a]
        return spread_copy(a, d, h, first_sem.at[a, h])

    def second_copy(a, h):
        d = (2 - h, 2, 1)[a]
        return spread_copy(a, d, h, second_sem.at[a, h if a == 0 else 0])

    def onward_copy(a, h):
        d = (1 + h, 1, 2)[a]
        return remote(
            spread.at[a, d, half(h), :], spread.at[a, 3, half(h), :],
            send_sem.at[4], onward_sem.at[min(a, 1)], (section, row_peer(3 - d), col),
        )

    def spread_grads(h):
        for a in (1, 2):
            first_copy(a, h).start()
        for a in (2, 1):
            second_copy(a, h).start()

    def relay_grads(h):
        for a in (1, 2):
            first_copy(a, h).wait_recv()
            onward_copy(a, h).start()

    def spread_hidden():
        for h in range(2):
            first_copy(0, h).start()
        for h in (1, 0):
            second_copy(0, h).start()

    def relay_hidden():
        for h in range(2):
            first_copy(0, h).wait_recv()
            onward_copy(0, h).start()

    def cross_copy(step, i, h):
        source, target = ((part_send.at[2], part_recv.at[2]), (middle.at[0], middle.at[1]))[step]
        return remote(
            source.at[i, half(h), :], target.at[i, half(h), :],
            send_sem.at[7 + step], cross_sem.at[step, i], (section, row_peer(1 + (step + h) % 2), col),
        )

    def branch_copy(d, c):
        return remote(
            branch_send.at[c, d], branch_recv.at[c, d], send_sem.at[5], branch_recv_sem.at[c], (section, row, behind(d))
        )

    far_outs = (own_out, far_out_1, far_out_2, far_out_3)

    def far_copy(d, c):
        return pltpu.make_async_copy(branch_send.at[c, d], far_outs[d].at[:, block_of(c)], out_sem.at[3])

    def store_copy(a, d):
        return pltpu.make_async_copy(spread.at[a, d], packed_out.at[a, :, piece_of(d)], out_sem.at[0])

    x_store = pltpu.make_async_copy(x_whole, x_out, out_sem.at[1])

    def dy_store(c):
        return pltpu.make_async_copy(dy_whole.at[:, block_of(c)], dy_out.at[:, block_of(c)], out_sem.at[2])

    def merge(slots):
        for d in range(4):
            for t in range(local):
                first = d * group + t * micro
                stage[first:first + micro, :slots.shape[3]] = slots[d, t].astype(jnp.float32)

    x_load = pltpu.make_async_copy(x_ref, x_slots.at[0], in_sem.at[0])

    def top_load(c):
        return pltpu.make_async_copy(top_ref.at[:, :, block_of(c)], dy_slots.at[c, 0], in_sem.at[1 + c])

    x_load.start()

    @pl.when(is_top)
    def _():
        for c in range(2):
            top_load(c).start()

    barrier = pltpu.get_barrier_semaphore()
    greeted = [(section, row, ahead(d)) for d in (1, 2, 3)]
    greeted += [(section, row_peer(d), col) for d in (1, 2, 3)]
    greeted += [(1 - section, row, ahead(d)) for d in range(4)]
    for device in greeted:
        pl.semaphore_signal(barrier, inc=1, device_id=device, device_id_type=ORDER)
    x_load.wait()

    @pl.when(is_top)
    def _():
        for c in range(2):
            top_load(c).wait()

    for a in range(3):
        weight_load(a)

    pl.semaphore_wait(barrier, len(greeted))

    def partner_go(which):
        pl.semaphore_signal(
            go_sem.at[which], inc=1, device_id=(1 - section, row, col), device_id_type=ORDER
        )

    @pl.when(is_bottom)
    def _():
        pl.semaphore_wait(go_sem.at[0], 1)

    for d in (2, 1, 3):
        x_copy(d).start()

    @pl.when(is_top)
    def _():
        for c in range(2):
            for d in (2, 1, 3):
                dy_copy(d, c).start()

    received(x_slots.at[pl.ds(1, 3)], x_recv_sem.at[0])
    merge(x_slots)

    @pl.when(is_top)
    def _():
        partner_go(0)

    x_whole[...] = stage[...].astype(jnp.bfloat16)
    x_store.start()
    for a in range(2):
        weight_wait(a)

    def forward_step(i, carry):
        d = 3 - i
        for a, weight in enumerate((w_gate, w_up)):
            part_send[a, d] = jnp.dot(
                x_whole[...], weight[:, piece_of(d)], preferred_element_type=jnp.float32
            ).astype(jnp.bfloat16)

            @pl.when(jnp.logical_and(is_top, d == 3))
            def _():
                for h in range(2):
                    via_copy(a, h).start()

            @pl.when(jnp.logical_and(is_top, d == 1 + a))
            def _():
                for h in range(2):
                    pair_copy(a, 1 + a, h).start()
        return carry

    lax.fori_loop(0, 4, forward_step, 0)

    def summed(a, where):
        total = part_send[a, 0, where, :].astype(jnp.float32)
        for d in range(1, 4 if a == 2 else 3):
            total = total + part_recv[a, d, where, :].astype(jnp.float32)
        return total

    def rows_of(i):
        return pl.ds(pl.multiple_of(i * 16, 16), 16)

    def sum_step(i, carry):
        where = rows_of(i)
        spread[1, 0, where, :] = summed(0, where).astype(jnp.bfloat16)
        spread[2, 0, where, :] = summed(1, where).astype(jnp.bfloat16)
        return carry

    def hidden_step(i, carry):
        where = rows_of(i)
        gate, up = summed(0, where), summed(1, where)
        gate_sum[where, :] = gate
        up_sum[where, :] = up
        spread[0, 0, where, :] = (gate * jax.nn.sigmoid(gate) * up).astype(jnp.bfloat16)
        return carry

    def factor_rows(first, count):
        def step(k, carry):
            d = first + k // (2 * steps)
            where = rows_of(k % (2 * steps))
            gate = spread[1, d, where, :].astype(jnp.float32)
            up = spread[2, d, where, :].astype(jnp.float32)
            sigmoid_gate = jax.nn.sigmoid(gate)
            activated = gate * sigmoid_gate
            slope = sigmoid_gate * (1.0 + gate * (1.0 - sigmoid_gate))
            spread[0, d, where, :] = (activated * up).astype(jnp.bfloat16)
            factors[0, d, where, :] = up * slope
            factors[1, d, where, :] = activated
            return carry

        lax.fori_loop(0, count * 2 * steps, step, 0)
        for d in range(first, first + count):
            store_copy(0, d).start()

    def grad_step(i, carry):
        where = rows_of(i)
        hidden_grad = summed(2, where)
        gate, up = gate_sum[where, :], up_sum[where, :]
        sigmoid_gate = jax.nn.sigmoid(gate)
        slope = sigmoid_gate * (1.0 + gate * (1.0 - sigmoid_gate))
        spread[1, 0, where, :] = (hidden_grad * up * slope).astype(jnp.bfloat16)
        spread[2, 0, where, :] = (hidden_grad * (gate * sigmoid_gate)).astype(jnp.bfloat16)
        return carry

    steps = span // 16

    def hidden_rows(h):
        received(part_recv.at[pl.ds(0, 2), pl.ds(1, 2), half(h), :], pair_sem.at[h])
        lax.fori_loop(h * steps, (h + 1) * steps, hidden_step, 0)

    def grad_rows(h):
        received(part_recv.at[2, pl.ds(1, 3), half(h), :], last_part_sem.at[h])
        lax.fori_loop(h * steps, (h + 1) * steps, grad_step, 0)
        spread_grads(h)

    @pl.when(is_bottom)
    def _():
        strip = 256 if turned.shape[1] % 256 == 0 else 128

        def turn(k, inner):
            cols = pl.ds(pl.multiple_of(k * strip, strip), strip)
            for a, weight in enumerate((w_gate, w_up)):
                turned[a, cols, :] = weight[:, cols].T
            return inner

        lax.fori_loop(0, turned.shape[1] // strip, turn, 0)
        pl.semaphore_wait(go_sem.at[1], 1)
        for h in range(2):
            for a in range(2):
                via_copy(a, h).start()
        for h in range(2):
            for a in range(2):
                pair_copy(a, 1 + a, h).start()

    for a in range(2):
        relay_sum(a, 0)

    @pl.when(is_bottom)
    def _():
        for a in range(2):
            relay_sum(a, 1)
        for h in range(2):
            received(part_recv.at[pl.ds(0, 2), pl.ds(1, 2), half(h), :], pair_sem.at[h])
            lax.fori_loop(h * steps, (h + 1) * steps, sum_step, 0)
            spread_grads(h)
        relay_grads(0)

    def merge_block(c):
        @pl.when(is_top)
        def _():
            received(dy_slots.at[c, pl.ds(1, 3)], dy_recv_sem.at[c])

        @pl.when(is_bottom)
        def _():
            received(dy_slots.at[c], dy_recv_sem.at[c])

        merge(dy_slots.at[c])
        dy_whole[:, c * block:(c + 1) * block] = stage[:, :block].astype(jnp.bfloat16)
        dy_store(c).start()

    weight_wait(2)

    for c in range(2):
        merge_block(c)

    def grad_terms_step(i, carry):
        d = section * (3 - i) + (1 - section) * i
        owner = section * row_peer(d) + (1 - section) * i
        piece = pl.ds(pl.multiple_of(owner * width, width), width)
        part_send[2, d] = lax.dot_general(
            dy_whole[...], w_down[piece, :], CONTRACT_COLS, preferred_element_type=jnp.float32
        ).astype(jnp.bfloat16)

        @pl.when(is_bottom)
        def _():
            for h in range(2):
                cross_copy(0, i, h).start()

        @pl.when(jnp.logical_and(is_top, d > 0))
        def _():
            last_part_copy(d, 0).start()

        @pl.when(jnp.logical_and(is_top, i == 1))
        def _():
            for a in range(2):
                relay_sum(a, 1)
        return carry

    lax.fori_loop(0, 4, grad_terms_step, 0)

    @pl.when(is_top)
    def _():
        for d in (3, 2, 1):
            last_part_copy(d, 1).start()
        for h in range(2):
            hidden_rows(h)
        for h in range(2):
            grad_rows(h)

    def send_branch(c):
        for d in (2, 3, 1, 0):
            first = d * group
            branch_send[c, d] = branch[first:first + group, c * block:(c + 1) * block].astype(jnp.bfloat16)
            if d:
                @pl.when(is_top)
                def _():
                    branch_copy(d, c).start()
            far_copy(d, c).start()

    def branch_terms(d, cols):
        return lax.dot_general(
            spread[1, d], w_gate[cols, piece_of(d)], CONTRACT_COLS, preferred_element_type=jnp.float32
        ) + lax.dot_general(
            spread[2, d], w_up[cols, piece_of(d)], CONTRACT_COLS, preferred_element_type=jnp.float32
        )

    def branch_step(d, carry):
        @pl.when(d == 1)
        def _():
            for h in range(2):
                relay_grads(h)
            partner_go(1)
            received(spread.at[2, 1], second_sem.at[2, 0])

        @pl.when(d == 2)
        def _():
            received(spread.at[1, 2], second_sem.at[1, 0])

        term = branch_terms(d, slice(None))

        @pl.when(d == 0)
        def _():
            branch[...] = term

        @pl.when(d > 0)
        def _():
            branch[...] += term
        return carry

    def last_branch_step(c, carry):
        @pl.when(c == 1)
        def _():
            send_branch(0)

        branch[:, block_of(c)] += branch_terms(3, block_of(c))
        return carry

    def finish_hidden():
        for h in range(2):
            second_copy(0, h).wait_recv()
        received(spread.at[0, 3], onward_sem.at[0])
        for d in range(4):
            store_copy(0, d).start()

    @pl.when(is_top)
    def _():
        lax.fori_loop(0, 3, branch_step, 0)
        received(spread.at[pl.ds(1, 2), 3], onward_sem.at[1])
        lax.fori_loop(0, 2, last_branch_step, 0)

    def cross_sum(i):
        received(part_recv.at[2, i], cross_sem.at[0, i])
        total = part_send[2, i].astype(jnp.float32) + part_recv[2, i].astype(jnp.float32)
        middle[0, i] = total.astype(jnp.bfloat16)
        for h in range(2):
            cross_copy(1, i, h).start()

    def cross_step(i, carry):
        received(middle.at[1, i], cross_sem.at[1, i])
        d = row_peer(i)

        def grads(k, inner):
            where = rows_of(k)
            hidden_grad = middle[0, i, where, :].astype(jnp.float32) + middle[1, i, where, :].astype(jnp.float32)
            for a in range(2):
                spread[1 + a, d, where, :] = (hidden_grad * factors[a, d, where, :]).astype(jnp.bfloat16)
            return inner

        lax.fori_loop(0, 2 * steps, grads, 0)
        for a in (1, 2):
            store_copy(a, d).start()
        term = jnp.dot(spread[1, d], turned[0, piece_of(d), :], preferred_element_type=jnp.float32)
        term = term + jnp.dot(spread[2, d], turned[1, piece_of(d), :], preferred_element_type=jnp.float32)

        @pl.when(i == 0)
        def _():
            branch[...] = term

        @pl.when(i > 0)
        def _():
            branch[...] += term
        return carry

    @pl.when(is_bottom)
    def _():
        relay_grads(1)
        received(spread.at[2, 1], second_sem.at[2, 0])
        received(spread.at[1, 2], second_sem.at[1, 0])
        factor_rows(0, 3)
        for i in range(4):
            cross_sum(i)
        received(spread.at[pl.ds(1, 2), 3], onward_sem.at[1])
        factor_rows(3, 1)
        sent(spread.at[pl.ds(1, 2), pl.ds(1, 2)], 3)
        sent(spread.at[pl.ds(1, 2), 3], 4)
        lax.fori_loop(0, 4, cross_step, 0)
        send_branch(0)

    send_branch(1)

    @pl.when(is_top)
    def _():
        for c in range(2):
            total = dy_whole[:group, c * block:(c + 1) * block].astype(jnp.float32) + branch[:group, c * block:(c + 1) * block]
            received(branch_recv.at[c, pl.ds(1, 3)], branch_recv_sem.at[c])
            for d in (1, 2, 3):
                total = total + branch_recv[c, d].astype(jnp.float32)
            stage[:group, :block] = total
            for t in range(local):
                result[c, t] = stage[t * micro:(t + 1) * micro, :block].astype(jnp.bfloat16)
            for d in (2, 3, 1, 0):
                pass_copy(d, c).start()
        for a in (1, 2):
            for d in range(4):
                store_copy(a, d).start()
        spread_hidden()
        relay_hidden()
        finish_hidden()
        sent(dy_slots.at[:, pl.ds(1, 3)], 1)
        sent(dy_slots, 6)
        sent(branch_send.at[:, pl.ds(1, 3)], 5)
        sent(part_send.at[:, pl.ds(1, 3)], 2)
        sent(spread.at[:, pl.ds(1, 2)], 3)
        sent(spread.at[:, 3], 4)

    @pl.when(is_bottom)
    def _():
        sent(part_send.at[pl.ds(0, 2), pl.ds(1, 3)], 2)
        sent(part_send.at[2], 7)
        sent(middle.at[0], 8)

    sent(x_slots.at[pl.ds(1, 3)], 0)
    pltpu.make_async_copy(spread, spread, out_sem.at[0]).wait()
    x_store.wait()
    pltpu.make_async_copy(dy_whole, dy_whole, out_sem.at[2]).wait()
    pltpu.make_async_copy(branch_send, branch_send, out_sem.at[3]).wait()


def update_kernel(
    x_ref, dy_ref, packed_ref, gate_out, up_out, down_out,
    x_held, dy_held, packed_held, gate_tiles, up_tiles, down_tiles, in_sem, sem,
):
    loads = [
        pltpu.make_async_copy(x_ref, x_held, in_sem.at[0]),
        pltpu.make_async_copy(packed_ref.at[1], packed_held.at[1], in_sem.at[1]),
        pltpu.make_async_copy(packed_ref.at[2], packed_held.at[2], in_sem.at[2]),
        pltpu.make_async_copy(packed_ref.at[0], packed_held.at[0], in_sem.at[3]),
        pltpu.make_async_copy(dy_ref, dy_held, in_sem.at[4]),
    ]
    for load in loads:
        load.start()

    def tiles_of(left, right, tiles, target, done):
        size = tiles.shape[1]

        def step(j, carry):
            where = pl.ds(pl.multiple_of(j * size, size), size)
            tiles[j] = lax.dot_general(left[:, where], right[...], CONTRACT_ROWS, preferred_element_type=jnp.float32)
            pltpu.make_async_copy(tiles.at[j], target.at[where, :], done).start()
            return carry

        lax.fori_loop(0, tiles.shape[0], step, 0)

    loads[0].wait()
    loads[1].wait()
    tiles_of(x_held, packed_held.at[1], gate_tiles, gate_out, sem.at[0])
    loads[2].wait()
    tiles_of(x_held, packed_held.at[2], up_tiles, up_out, sem.at[1])
    loads[3].wait()
    loads[4].wait()
    tiles_of(packed_held.at[0], dy_held, down_tiles, down_out, sem.at[2])
    for a, tiles in enumerate((gate_tiles, up_tiles, down_tiles)):
        pltpu.make_async_copy(tiles, tiles, sem.at[a]).wait()


def weight_updates(x_whole, dy_whole, packed):
    rows, width = x_whole.shape
    hidden_width = packed.shape[2]
    tall, wide = (next(t for t in (256, 128) if n % t == 0) for n in (hidden_width, width))
    f32 = jnp.float32
    hbm = pl.BlockSpec(memory_space=pltpu.HBM)
    return pl.pallas_call(
        update_kernel,
        out_shape=(
            jax.ShapeDtypeStruct((width, hidden_width), f32),
            jax.ShapeDtypeStruct((width, hidden_width), f32),
            jax.ShapeDtypeStruct((hidden_width, width), f32),
        ),
        in_specs=[hbm, hbm, hbm],
        out_specs=(hbm, hbm, hbm),
        scratch_shapes=[
            pltpu.VMEM((rows, width), jnp.bfloat16),
            pltpu.VMEM((rows, width), jnp.bfloat16),
            pltpu.VMEM((3, rows, hidden_width), jnp.bfloat16),
            pltpu.VMEM((width // wide, wide, hidden_width), f32),
            pltpu.VMEM((width // wide, wide, hidden_width), f32),
            pltpu.VMEM((hidden_width // tall, tall, width), f32),
            pltpu.SemaphoreType.DMA((5,)),
            pltpu.SemaphoreType.DMA((3,)),
        ],
        compiler_params=pltpu.CompilerParams(vmem_limit_bytes=67043328),
        cost_estimate=pl.CostEstimate(
            flops=6 * rows * width * hidden_width,
            bytes_accessed=12 * width * hidden_width + 2 * rows * (2 * width + 3 * hidden_width),
            transcendentals=0,
        ),
    )(x_whole, dy_whole, packed)


def fast_shards(section_inputs, out_grad, gate_weight, up_weight, down_weight):
    panels = section_inputs[0]
    micro, local, width = panels.shape
    group = micro * local
    held = (local, micro, width)
    rows = group * lax.axis_size("col")
    hidden_width = gate_weight.shape[2]
    piece = hidden_width // lax.axis_size("row")
    hbm = pl.BlockSpec(memory_space=pltpu.HBM)
    bf16, f32 = jnp.bfloat16, jnp.float32
    dma = pltpu.SemaphoreType.DMA
    block = width // 2
    far = jax.ShapeDtypeStruct((group, width), bf16)
    x_whole, dy_whole, packed, own, *far_terms = pl.pallas_call(
        relay_kernel,
        out_shape=(
            jax.ShapeDtypeStruct((rows, width), bf16),
            jax.ShapeDtypeStruct((rows, width), bf16),
            jax.ShapeDtypeStruct((3, rows, hidden_width), bf16),
            far, far, far, far,
        ),
        in_specs=[hbm] * 5,
        out_specs=(hbm,) * 7,
        scratch_shapes=[
            pltpu.VMEM((width, hidden_width), bf16),
            pltpu.VMEM((width, hidden_width), bf16),
            pltpu.VMEM((hidden_width, width), bf16),
            pltpu.VMEM((2, hidden_width, width), bf16),
            pltpu.VMEM((4, *held), bf16),
            pltpu.VMEM((2, 4, local, micro, block), bf16),
            pltpu.VMEM((rows, width), bf16),
            pltpu.VMEM((rows, width), bf16),
            pltpu.VMEM((rows, width), f32),
            pltpu.VMEM((3, 4, rows, piece), bf16),
            pltpu.VMEM((3, 4, rows, piece), bf16),
            pltpu.VMEM((3, 4, rows, piece), bf16),
            pltpu.VMEM((rows, piece), f32),
            pltpu.VMEM((rows, piece), f32),
            pltpu.VMEM((2, 4, rows, piece), f32),
            pltpu.VMEM((2, 4, rows, piece), bf16),
            pltpu.VMEM((rows, width), f32),
            pltpu.VMEM((2, 4, group, block), bf16),
            pltpu.VMEM((2, 4, group, block), bf16),
            pltpu.VMEM((2, local, micro, block), bf16),
            dma((3,)), dma((3,)), dma((9,)), dma((1,)), dma((2,)), dma((2, 2)), dma((2,)), dma((2,)),
            dma((3, 2)), dma((3, 2)), dma((2,)), dma((2, 4)), dma((2,)), dma((4,)), pltpu.SemaphoreType.REGULAR((2,)),
        ],
        compiler_params=pltpu.CompilerParams(collective_id=0, has_side_effects=True, vmem_limit_bytes=60 * 2**20),
    )(
        panels.transpose(1, 0, 2), out_grad.transpose(1, 0, 2),
        gate_weight[0], up_weight[0], down_weight[0],
    )
    cols = lax.axis_size("col")
    arrived = [
        lax.ppermute(term, "col", [(i, (i + cols - d) % cols) for i in range(cols)])
        for d, term in zip((1, 2, 3), far_terms, strict=True)
    ]
    grads = weight_updates(x_whole, dy_whole, packed)
    grad = dy_whole[:group].astype(f32) + own.astype(f32)
    for term in arrived:
        grad = grad + term.astype(f32)
    grad = grad.astype(bf16).reshape(held).transpose(1, 0, 2)
    return (grad[None], *(g[None] for g in grads))


def fits_kernel(mesh, gate_weight, section_inputs):
    sizes = mesh.shape
    if (sizes["section"], sizes["row"], sizes["col"]) != (2, 4, 4):
        return False
    piece = gate_weight.shape[2] // (sizes["row"] * sizes["col"])
    local = section_inputs.shape[1] * section_inputs.shape[2] // sizes["col"]
    return piece % 128 == 0 and section_inputs.shape[3] % (256 * sizes["row"]) == 0 and local % 8 == 0 and (local * sizes["col"]) % 32 == 0


def solution(mesh):
    specs = dict(
        mesh=mesh,
        in_specs=(
            P("section", None, "col", "row"),
            P(None, "col", "row"),
            P("section", "row", "col"),
            P("section", "row", "col"),
            P("section", "col", "row"),
        ),
        out_specs=(
            P("section", None, "col", "row"),
            P("section", "row", "col"),
            P("section", "row", "col"),
            P("section", "col", "row"),
        ),
        check_vma=False,
    )

    def run(section_inputs, out_grad, gate_weight, up_weight, down_weight):
        body = fast_shards if fits_kernel(mesh, gate_weight, section_inputs) else shards
        return jax.shard_map(body, **specs)(section_inputs, out_grad, gate_weight, up_weight, down_weight)

    return run
```

```python
import jax
import jax.numpy as jnp
from jax import lax
from jax.experimental import pallas as pl
from jax.experimental.pallas import tpu as pltpu
from jax.sharding import PartitionSpec as P

CONTRACT_ROWS = (((0,), (0,)), ((), ()))
CONTRACT_COLS = (((1,), (1,)), ((), ()))


def passed_along(block, axis, distance):
    devices = range(lax.axis_size(axis))
    route = [(i - distance, i) for i in devices if i - distance in devices]
    return lax.ppermute(block, axis, route)


def spread_panel(panel):
    return lax.all_gather(panel, "col", axis=0, tiled=True)


def row_partials(make_terms, keep_rows):
    return lax.psum_scatter(
        make_terms(jnp.int32(0), keep_rows * lax.axis_size("row")).astype(jnp.bfloat16),
        "row",
        scatter_dimension=0,
        tiled=True,
    ).astype(jnp.float32)


def layer_backward(x_local, dy_local, w_both, w_down):
    hidden_width = w_down.shape[0]
    x_whole = spread_panel(x_local)
    dy_whole = spread_panel(dy_local)
    keep_rows = x_whole.shape[0] // lax.axis_size("row")

    def forward_terms(first_row, row_count):
        return jnp.dot(x_whole, w_both, preferred_element_type=jnp.float32)

    def backward_terms(first_row, row_count):
        return lax.dot_general(dy_whole, w_down, CONTRACT_COLS, preferred_element_type=jnp.float32)

    both_sums = row_partials(forward_terms, keep_rows)
    hidden_grad = row_partials(backward_terms, keep_rows)
    gate_sum = both_sums[:, :hidden_width]
    up_sum = both_sums[:, hidden_width:]
    sigmoid_gate = jax.nn.sigmoid(gate_sum)
    activated = gate_sum * sigmoid_gate
    slope = sigmoid_gate * (1.0 + gate_sum * (1.0 - sigmoid_gate))
    hidden = (activated * up_sum).astype(jnp.bfloat16)
    gate_grad = (hidden_grad * up_sum * slope).astype(jnp.bfloat16)
    up_grad = (hidden_grad * activated).astype(jnp.bfloat16)
    packed = jnp.concatenate([hidden, gate_grad, up_grad], axis=1)
    gathered = lax.all_gather(packed, "row", axis=0, tiled=True)
    hidden_whole = gathered[:, :hidden_width]
    both_grads = gathered[:, hidden_width:]
    branch_sum = lax.psum_scatter(
        lax.dot_general(
            both_grads, w_both, CONTRACT_COLS, preferred_element_type=jnp.float32
        ).astype(jnp.bfloat16),
        "col",
        scatter_dimension=0,
        tiled=True,
    ).astype(jnp.float32)
    input_grad = (dy_local.astype(jnp.float32) + branch_sum).astype(jnp.bfloat16)
    down_update = lax.dot_general(
        hidden_whole, dy_whole, CONTRACT_ROWS, preferred_element_type=jnp.float32
    )
    both_update = lax.dot_general(
        x_whole, both_grads, CONTRACT_ROWS, preferred_element_type=jnp.float32
    )
    return (input_grad, both_update, down_update)


def shards(section_inputs, out_grad, gate_weight, up_weight, down_weight):
    section_id = lax.axis_index("section")
    last_section = lax.axis_size("section") - 1
    is_last = section_id == last_section
    panels = section_inputs[0]
    w_both = jnp.concatenate([gate_weight[0], up_weight[0]], axis=1)
    w_down = down_weight[0]
    hidden_width = w_down.shape[0]
    micro_count = panels.shape[0]
    both_total = jnp.zeros(w_both.shape, jnp.float32)
    down_total = jnp.zeros(w_down.shape, jnp.float32)
    merged_shape = (micro_count * panels.shape[1], panels.shape[2])
    x_local = panels.reshape(merged_shape)
    top_grads = out_grad.reshape(merged_shape)
    received = jnp.zeros(merged_shape, jnp.bfloat16)
    merged_results = received
    for step_index in range(last_section + 1):
        is_active = section_id == last_section - step_index
        dy_local = jnp.where(is_last, top_grads, received)
        input_grad, both_update, down_update = layer_backward(x_local, dy_local, w_both, w_down)
        merged_results = jnp.where(is_active, input_grad, merged_results)
        both_total = both_total + jnp.where(is_active, both_update, 0.0)
        down_total = down_total + jnp.where(is_active, down_update, 0.0)
        if step_index < last_section:
            received = passed_along(input_grad, "section", -1)
    results = merged_results.reshape(panels.shape)
    return (
        results[None],
        both_total[:, :hidden_width][None],
        both_total[:, hidden_width:][None],
        down_total[None],
    )


ORDER = pl.DeviceIdType.MESH


def remote(src, dst, send_sem, recv_sem, target):
    return pltpu.make_async_remote_copy(
        src_ref=src, dst_ref=dst, send_sem=send_sem, recv_sem=recv_sem, device_id=target, device_id_type=ORDER
    )


def relay_kernel(
    x_ref, top_ref, gate_ref, up_ref, down_ref,
    x_whole, dy_whole, spread, result,
    w_gate, w_up, w_down, turned, x_slots, dy_slots, stage, part_send, part_recv, gate_sum, up_sum, factors, middle,
    branch, branch_send, branch_recv,
    w_sem, in_sem, send_sem, x_recv_sem, dy_recv_sem, via_sem, pair_sem, last_part_sem,
    first_sem, second_sem, onward_sem, cross_sem, branch_recv_sem, go_sem,
):
    section = lax.axis_index("section")
    row = lax.axis_index("row")
    col = lax.axis_index("col")
    rows, width = part_send.shape[2], part_send.shape[3]
    local, micro = x_slots.shape[1:3]
    span = rows // 2
    group = local * micro
    block = x_slots.shape[3] // 2
    own = row
    is_top = section == 1
    is_bottom = section == 0

    def row_peer(d):
        hi, lo = row // 2, row % 2
        return ((hi + d // 2) % 2) * 2 + (lo + d % 2) % 2

    def ahead(d):
        return (col + d) % 4

    def behind(d):
        return (col + 4 - d) % 4

    def half(h):
        return pl.ds(h * span, span)

    def block_of(c):
        return pl.ds(pl.multiple_of(c * block, block), block)

    def piece_of(d):
        return pl.ds(pl.multiple_of(row_peer(d) * width, width), width)

    weights = ((gate_ref, w_gate), (up_ref, w_up), (down_ref, w_down))

    def weight_load(a):
        source, target = weights[a]
        size = target.shape[0] // 4
        for q in range(4):
            where = pl.ds(q * size, size)
            pltpu.make_async_copy(source.at[where, :], target.at[where, :], w_sem.at[a]).start()

    def weight_wait(a):
        source, target = weights[a]
        pltpu.make_async_copy(source, target, w_sem.at[a]).wait()

    def received(ref, sem):
        remote(ref, ref, send_sem.at[0], sem, (section, row, ahead(1))).wait_recv()

    def sent(ref, kind):
        remote(ref, ref, send_sem.at[kind], send_sem.at[kind], (section, row, ahead(1))).wait_send()

    def x_copy(d):
        return remote(x_slots.at[0], x_slots.at[d], send_sem.at[0], x_recv_sem.at[0], (section, row, ahead(d)))

    def dy_copy(d, c):
        return remote(
            dy_slots.at[c, 0], dy_slots.at[c, d], send_sem.at[1], dy_recv_sem.at[c], (section, row, ahead(d))
        )

    def pass_copy(d, c):
        return remote(result.at[:, :, block_of(c)], dy_slots.at[c, d], send_sem.at[6], dy_recv_sem.at[c], (0, row, ahead(d)))

    def part_copy(a, d, h, via, sem):
        place = (a, d, half(h), slice(None))
        return remote(
            part_send.at[place], part_recv.at[place], send_sem.at[2], sem, (section, row_peer(via), col)
        )

    def via_copy(a, h):
        return part_copy(a, 3, h, 1 + a, via_sem.at[a, h])

    def pair_copy(a, d, h):
        return part_copy(a, d, h, d, pair_sem.at[h])

    def last_part_copy(d, h):
        return part_copy(2, d, h, d, last_part_sem.at[h])

    def relay_sum(a, h):
        middle = 2 - a
        via_copy(a, h).wait_recv()
        total = part_send[a, middle, half(h), :].astype(jnp.float32) + part_recv[a, 3, half(h), :].astype(jnp.float32)
        part_send[a, middle, half(h), :] = total.astype(jnp.bfloat16)
        pair_copy(a, middle, h).start()

    def spread_copy(a, piece, d, h, sem):
        place = (a, piece, half(h), slice(None))
        return remote(spread.at[place], spread.at[place], send_sem.at[3], sem, (section, row_peer(d), col))

    def first_copy(a, h, piece=None):
        d = (1 + h, 1, 2)[a]
        return spread_copy(a, own if piece is None else row_peer(d), d, h, first_sem.at[a, h])

    def second_copy(a, h, piece=None):
        d = (2 - h, 2, 1)[a]
        return spread_copy(a, own if piece is None else row_peer(d), d, h, second_sem.at[a, h if a == 0 else 0])

    def onward_copy(a, h):
        d = (1 + h, 1, 2)[a]
        return remote(
            spread.at[a, row_peer(d), half(h), :], spread.at[a, row_peer(d), half(h), :],
            send_sem.at[4], onward_sem.at[min(a, 1)], (section, row_peer(3 - d), col),
        )

    def spread_grads(h):
        for a in (1, 2):
            first_copy(a, h).start()
        for a in (2, 1):
            second_copy(a, h).start()

    def relay_grads(h):
        for a in (1, 2):
            first_copy(a, h, 1).wait_recv()
            onward_copy(a, h).start()

    def spread_hidden():
        for h in range(2):
            first_copy(0, h).start()
        for h in (1, 0):
            second_copy(0, h).start()

    def relay_hidden():
        for h in range(2):
            first_copy(0, h, 1).wait_recv()
            onward_copy(0, h).start()

    def cross_copy(step, i, h):
        source, target = ((part_send.at[2], part_recv.at[2]), (middle.at[0], middle.at[1]))[step]
        return remote(
            source.at[i, half(h), :], target.at[i, half(h), :],
            send_sem.at[7 + step], cross_sem.at[step, i], (section, row_peer(1 + (step + h) % 2), col),
        )

    def branch_copy(d, c):
        return remote(
            branch_send.at[c, d], branch_recv.at[c, d], send_sem.at[5], branch_recv_sem.at[c], (section, row, behind(d))
        )

    def merge(slots):
        for d in range(4):
            for t in range(local):
                first = d * group + t * micro
                stage[first:first + micro, :slots.shape[3]] = slots[d, t].astype(jnp.float32)

    x_load = pltpu.make_async_copy(x_ref, x_slots.at[0], in_sem.at[0])

    def top_load(c):
        return pltpu.make_async_copy(top_ref.at[:, :, block_of(c)], dy_slots.at[c, 0], in_sem.at[1 + c])

    x_load.start()

    @pl.when(is_top)
    def _():
        for c in range(2):
            top_load(c).start()

    barrier = pltpu.get_barrier_semaphore()
    greeted = [(section, row, ahead(d)) for d in (1, 2, 3)]
    greeted += [(section, row_peer(d), col) for d in (1, 2, 3)]
    greeted += [(1 - section, row, ahead(d)) for d in range(4)]
    for device in greeted:
        pl.semaphore_signal(barrier, inc=1, device_id=device, device_id_type=ORDER)
    x_load.wait()

    @pl.when(is_top)
    def _():
        for c in range(2):
            top_load(c).wait()

    for a in range(3):
        weight_load(a)

    pl.semaphore_wait(barrier, len(greeted))

    def partner_go(which):
        pl.semaphore_signal(
            go_sem.at[which], inc=1, device_id=(1 - section, row, col), device_id_type=ORDER
        )

    @pl.when(is_bottom)
    def _():
        pl.semaphore_wait(go_sem.at[0], 1)

    for d in (2, 1, 3):
        x_copy(d).start()

    @pl.when(is_top)
    def _():
        for c in range(2):
            for d in (2, 1, 3):
                dy_copy(d, c).start()

    received(x_slots.at[pl.ds(1, 3)], x_recv_sem.at[0])
    merge(x_slots)

    @pl.when(is_top)
    def _():
        partner_go(0)

    x_whole[...] = stage[...].astype(jnp.bfloat16)
    for a in range(2):
        weight_wait(a)

    def forward_step(i, carry):
        d = 3 - i
        for a, weight in enumerate((w_gate, w_up)):
            part_send[a, d] = jnp.dot(
                x_whole[...], weight[:, piece_of(d)], preferred_element_type=jnp.float32
            ).astype(jnp.bfloat16)

            @pl.when(jnp.logical_and(is_top, d == 3))
            def _():
                for h in range(2):
                    via_copy(a, h).start()

            @pl.when(jnp.logical_and(is_top, d == 1 + a))
            def _():
                for h in range(2):
                    pair_copy(a, 1 + a, h).start()
        return carry

    lax.fori_loop(0, 4, forward_step, 0)

    def summed(a, where):
        total = part_send[a, 0, where, :].astype(jnp.float32)
        for d in range(1, 4 if a == 2 else 3):
            total = total + part_recv[a, d, where, :].astype(jnp.float32)
        return total

    def rows_of(i):
        return pl.ds(pl.multiple_of(i * 16, 16), 16)

    def sum_step(i, carry):
        where = rows_of(i)
        spread[1, own, where, :] = summed(0, where).astype(jnp.bfloat16)
        spread[2, own, where, :] = summed(1, where).astype(jnp.bfloat16)
        return carry

    def hidden_step(i, carry):
        where = rows_of(i)
        gate, up = summed(0, where), summed(1, where)
        gate_sum[where, :] = gate
        up_sum[where, :] = up
        spread[0, own, where, :] = (gate * jax.nn.sigmoid(gate) * up).astype(jnp.bfloat16)
        return carry

    def factor_rows(first, count):
        def step(k, carry):
            d = row_peer(first + k // (2 * steps))
            where = rows_of(k % (2 * steps))
            gate = spread[1, d, where, :].astype(jnp.float32)
            up = spread[2, d, where, :].astype(jnp.float32)
            sigmoid_gate = jax.nn.sigmoid(gate)
            activated = gate * sigmoid_gate
            slope = sigmoid_gate * (1.0 + gate * (1.0 - sigmoid_gate))
            spread[0, d, where, :] = (activated * up).astype(jnp.bfloat16)
            factors[0, d, where, :] = up * slope
            factors[1, d, where, :] = activated
            return carry

        lax.fori_loop(0, count * 2 * steps, step, 0)

    def grad_step(i, carry):
        where = rows_of(i)
        hidden_grad = summed(2, where)
        gate, up = gate_sum[where, :], up_sum[where, :]
        sigmoid_gate = jax.nn.sigmoid(gate)
        slope = sigmoid_gate * (1.0 + gate * (1.0 - sigmoid_gate))
        spread[1, own, where, :] = (hidden_grad * up * slope).astype(jnp.bfloat16)
        spread[2, own, where, :] = (hidden_grad * (gate * sigmoid_gate)).astype(jnp.bfloat16)
        return carry

    steps = span // 16

    def hidden_rows(h):
        received(part_recv.at[pl.ds(0, 2), pl.ds(1, 2), half(h), :], pair_sem.at[h])
        lax.fori_loop(h * steps, (h + 1) * steps, hidden_step, 0)

    def grad_rows(h):
        received(part_recv.at[2, pl.ds(1, 3), half(h), :], last_part_sem.at[h])
        lax.fori_loop(h * steps, (h + 1) * steps, grad_step, 0)
        spread_grads(h)

    @pl.when(is_bottom)
    def _():
        strip = 256 if turned.shape[1] % 256 == 0 else 128

        def turn(k, inner):
            cols = pl.ds(pl.multiple_of(k * strip, strip), strip)
            for a, weight in enumerate((w_gate, w_up)):
                turned[a, cols, :] = weight[:, cols].T
            return inner

        lax.fori_loop(0, turned.shape[1] // strip, turn, 0)
        pl.semaphore_wait(go_sem.at[1], 1)
        for h in range(2):
            for a in range(2):
                via_copy(a, h).start()
        for h in range(2):
            for a in range(2):
                pair_copy(a, 1 + a, h).start()

    for a in range(2):
        relay_sum(a, 0)

    @pl.when(is_bottom)
    def _():
        for a in range(2):
            relay_sum(a, 1)
        for h in range(2):
            received(part_recv.at[pl.ds(0, 2), pl.ds(1, 2), half(h), :], pair_sem.at[h])
            lax.fori_loop(h * steps, (h + 1) * steps, sum_step, 0)
            spread_grads(h)
        relay_grads(0)

    def merge_block(c):
        @pl.when(is_top)
        def _():
            received(dy_slots.at[c, pl.ds(1, 3)], dy_recv_sem.at[c])

        @pl.when(is_bottom)
        def _():
            received(dy_slots.at[c], dy_recv_sem.at[c])

        merge(dy_slots.at[c])
        dy_whole[:, c * block:(c + 1) * block] = stage[:, :block].astype(jnp.bfloat16)

    weight_wait(2)

    for c in range(2):
        merge_block(c)

    def grad_terms_step(i, carry):
        d = section * (3 - i) + (1 - section) * i
        owner = section * row_peer(d) + (1 - section) * i
        piece = pl.ds(pl.multiple_of(owner * width, width), width)
        part_send[2, d] = lax.dot_general(
            dy_whole[...], w_down[piece, :], CONTRACT_COLS, preferred_element_type=jnp.float32
        ).astype(jnp.bfloat16)

        @pl.when(is_bottom)
        def _():
            for h in range(2):
                cross_copy(0, i, h).start()

        @pl.when(jnp.logical_and(is_top, d > 0))
        def _():
            last_part_copy(d, 0).start()

        @pl.when(jnp.logical_and(is_top, i == 1))
        def _():
            for a in range(2):
                relay_sum(a, 1)
        return carry

    lax.fori_loop(0, 4, grad_terms_step, 0)

    @pl.when(is_top)
    def _():
        for d in (3, 2, 1):
            last_part_copy(d, 1).start()
        for h in range(2):
            hidden_rows(h)
        for h in range(2):
            grad_rows(h)

    def send_branch(c):
        for d in (2, 3, 1):
            first = d * group
            branch_send[c, d] = branch[first:first + group, c * block:(c + 1) * block].astype(jnp.bfloat16)
            branch_copy(d, c).start()

    def branch_terms(d, cols):
        return lax.dot_general(
            spread[1, row_peer(d)], w_gate[cols, piece_of(d)], CONTRACT_COLS, preferred_element_type=jnp.float32
        ) + lax.dot_general(
            spread[2, row_peer(d)], w_up[cols, piece_of(d)], CONTRACT_COLS, preferred_element_type=jnp.float32
        )

    def branch_step(d, carry):
        @pl.when(d == 1)
        def _():
            for h in range(2):
                relay_grads(h)
            partner_go(1)
            received(spread.at[2, row_peer(1)], second_sem.at[2, 0])

        @pl.when(d == 2)
        def _():
            received(spread.at[1, row_peer(2)], second_sem.at[1, 0])

        term = branch_terms(d, slice(None))

        @pl.when(d == 0)
        def _():
            branch[...] = term

        @pl.when(d > 0)
        def _():
            branch[...] += term
        return carry

    def last_branch_step(c, carry):
        @pl.when(c == 1)
        def _():
            send_branch(0)

        branch[:, block_of(c)] += branch_terms(3, block_of(c))
        return carry

    def finish_hidden():
        for h in range(2):
            second_copy(0, h, 1).wait_recv()
        received(spread.at[0, row_peer(3)], onward_sem.at[0])

    @pl.when(is_top)
    def _():
        lax.fori_loop(0, 3, branch_step, 0)
        received(spread.at[pl.ds(1, 2), row_peer(3)], onward_sem.at[1])
        lax.fori_loop(0, 2, last_branch_step, 0)

    def cross_sum(i):
        received(part_recv.at[2, i], cross_sem.at[0, i])
        total = part_send[2, i].astype(jnp.float32) + part_recv[2, i].astype(jnp.float32)
        middle[0, i] = total.astype(jnp.bfloat16)
        for h in range(2):
            cross_copy(1, i, h).start()

    def cross_grads(i):
        received(middle.at[1, i], cross_sem.at[1, i])

        def grads(k, carry):
            where = rows_of(k)
            hidden_grad = middle[0, i, where, :].astype(jnp.float32) + middle[1, i, where, :].astype(jnp.float32)
            for a in range(2):
                spread[1 + a, i, where, :] = (hidden_grad * factors[a, i, where, :]).astype(jnp.bfloat16)
            return carry

        lax.fori_loop(0, 2 * steps, grads, 0)

    def turned_terms(i, cols):
        piece = pl.ds(i * width if isinstance(i, int) else pl.multiple_of(i * width, width), width)
        term = jnp.dot(spread[1, i], turned[0, piece, cols], preferred_element_type=jnp.float32)
        return term + jnp.dot(spread[2, i], turned[1, piece, cols], preferred_element_type=jnp.float32)

    def cross_step(i, carry):
        cross_grads(i)
        term = turned_terms(i, slice(None))

        @pl.when(i == 0)
        def _():
            branch[...] = term

        @pl.when(i > 0)
        def _():
            branch[...] += term
        return carry

    def last_cross_step(c, carry):
        @pl.when(c == 1)
        def _():
            send_branch(0)

        branch[:, block_of(c)] += turned_terms(3, block_of(c))
        return carry

    @pl.when(is_bottom)
    def _():
        relay_grads(1)
        received(spread.at[2, row_peer(1)], second_sem.at[2, 0])
        received(spread.at[1, row_peer(2)], second_sem.at[1, 0])
        factor_rows(0, 3)
        for i in range(4):
            cross_sum(i)
        partner_go(2)
        received(spread.at[pl.ds(1, 2), row_peer(3)], onward_sem.at[1])
        factor_rows(3, 1)
        sent(spread.at[pl.ds(1, 2), pl.ds(1, 2)], 3)
        sent(spread.at[pl.ds(1, 2), 3], 4)
        lax.fori_loop(0, 3, cross_step, 0)
        cross_grads(3)
        lax.fori_loop(0, 2, last_cross_step, 0)

    send_branch(1)

    for c in range(2):
        cols = slice(c * block, (c + 1) * block)
        total = dy_whole[:group, cols].astype(jnp.float32) + branch[:group, cols]
        received(branch_recv.at[c, pl.ds(1, 3)], branch_recv_sem.at[c])
        for d in (1, 2, 3):
            total = total + branch_recv[c, d].astype(jnp.float32)
        stage[:group, :block] = total
        for t in range(local):
            result[t, :, cols] = stage[t * micro:(t + 1) * micro, :block].astype(jnp.bfloat16)

        @pl.when(is_top)
        def _():
            for d in (2, 3, 1, 0):
                pass_copy(d, c).start()

    @pl.when(is_top)
    def _():
        pl.semaphore_wait(go_sem.at[2], 1)
        spread_hidden()
        relay_hidden()
        finish_hidden()
        sent(dy_slots.at[:, pl.ds(1, 3)], 1)
        sent(dy_slots, 6)
        sent(part_send.at[:, pl.ds(1, 3)], 2)
        sent(spread.at[:, pl.ds(1, 2)], 3)
        sent(spread.at[:, 3], 4)

    @pl.when(is_bottom)
    def _():
        sent(part_send.at[pl.ds(0, 2), pl.ds(1, 3)], 2)
        sent(part_send.at[2], 7)
        sent(middle.at[0], 8)

    sent(branch_send.at[:, pl.ds(1, 3)], 5)
    sent(x_slots.at[pl.ds(1, 3)], 0)

def update_kernel(x_ref, dy_ref, packed_ref, gate_out, up_out, down_out, wide_tiles, down_tiles, sem):
    pieces, rows, piece = packed_ref.shape[1:]
    tall = wide_tiles.shape[2]

    def wide_step(k, carry):
        a = k // wide_tiles.shape[1]
        j = k % wide_tiles.shape[1]
        where = pl.ds(pl.multiple_of(j * tall, tall), tall)

        for p in range(pieces):
            wide_tiles[a, j, :, p * piece:(p + 1) * piece] = lax.dot_general(
                x_ref[:, where], packed_ref[1 + a, p], CONTRACT_ROWS, preferred_element_type=jnp.float32
            )
        for b, target in enumerate((gate_out, up_out)):
            @pl.when(a == b)
            def _():
                pltpu.make_async_copy(wide_tiles.at[b, j], target.at[where, :], sem.at[b]).start()
        return carry

    lax.fori_loop(0, 2 * wide_tiles.shape[1], wide_step, 0)
    def down_step(p, carry):
        where = pl.ds(pl.multiple_of(p * piece, piece), piece)
        down_tiles[p] = lax.dot_general(
            packed_ref[0, p], dy_ref[...], CONTRACT_ROWS, preferred_element_type=jnp.float32
        )
        pltpu.make_async_copy(down_tiles.at[p], down_out.at[where, :], sem.at[2]).start()
        return carry

    lax.fori_loop(0, pieces, down_step, 0)
    for a, tiles in enumerate((wide_tiles.at[0], wide_tiles.at[1], down_tiles)):
        pltpu.make_async_copy(tiles, tiles, sem.at[a]).wait()


def weight_updates(x_whole, dy_whole, packed):
    rows, width = x_whole.shape
    pieces, piece = packed.shape[1], packed.shape[3]
    hidden_width = pieces * piece
    tall = 256 if width % 256 == 0 else 128
    f32 = jnp.float32
    vmem = pl.BlockSpec(memory_space=pltpu.VMEM)
    hbm = pl.BlockSpec(memory_space=pltpu.HBM)
    return pl.pallas_call(
        update_kernel,
        out_shape=(
            jax.ShapeDtypeStruct((width, hidden_width), f32),
            jax.ShapeDtypeStruct((width, hidden_width), f32),
            jax.ShapeDtypeStruct((hidden_width, width), f32),
        ),
        in_specs=[vmem, vmem, vmem],
        out_specs=(hbm, hbm, hbm),
        scratch_shapes=[
            pltpu.VMEM((2, width // tall, tall, hidden_width), f32),
            pltpu.VMEM((pieces, piece, width), f32),
            pltpu.SemaphoreType.DMA((3,)),
        ],
        compiler_params=pltpu.CompilerParams(vmem_limit_bytes=46 * 2**20),
        cost_estimate=pl.CostEstimate(
            flops=6 * rows * width * hidden_width,
            bytes_accessed=12 * width * hidden_width + 2 * rows * (2 * width + 3 * hidden_width),
            transcendentals=0,
        ),
    )(x_whole, dy_whole, packed)


def fast_shards(section_inputs, out_grad, gate_weight, up_weight, down_weight):
    panels = section_inputs[0]
    micro, local, width = panels.shape
    group = micro * local
    held = (local, micro, width)
    rows = group * lax.axis_size("col")
    hidden_width = gate_weight.shape[2]
    piece = hidden_width // lax.axis_size("row")
    hbm = pl.BlockSpec(memory_space=pltpu.HBM)
    vmem = pl.BlockSpec(memory_space=pltpu.VMEM)
    bf16, f32 = jnp.bfloat16, jnp.float32
    dma = pltpu.SemaphoreType.DMA
    block = width // 2
    x_whole, dy_whole, packed, grad = pl.pallas_call(
        relay_kernel,
        out_shape=(
            jax.ShapeDtypeStruct((rows, width), bf16),
            jax.ShapeDtypeStruct((rows, width), bf16),
            jax.ShapeDtypeStruct((3, 4, rows, piece), bf16),
            jax.ShapeDtypeStruct(held, bf16),
        ),
        in_specs=[hbm] * 5,
        out_specs=(vmem,) * 4,
        scratch_shapes=[
            pltpu.VMEM((width, hidden_width), bf16),
            pltpu.VMEM((width, hidden_width), bf16),
            pltpu.VMEM((hidden_width, width), bf16),
            pltpu.VMEM((2, hidden_width, width), bf16),
            pltpu.VMEM((4, *held), bf16),
            pltpu.VMEM((2, 4, local, micro, block), bf16),
            pltpu.VMEM((rows, width), f32),
            pltpu.VMEM((3, 4, rows, piece), bf16),
            pltpu.VMEM((3, 4, rows, piece), bf16),
            pltpu.VMEM((rows, piece), f32),
            pltpu.VMEM((rows, piece), f32),
            pltpu.VMEM((2, 4, rows, piece), f32),
            pltpu.VMEM((2, 4, rows, piece), bf16),
            pltpu.VMEM((rows, width), f32),
            pltpu.VMEM((2, 4, group, block), bf16),
            pltpu.VMEM((2, 4, group, block), bf16),
            dma((3,)), dma((3,)), dma((9,)), dma((1,)), dma((2,)), dma((2, 2)), dma((2,)), dma((2,)),
            dma((3, 2)), dma((3, 2)), dma((2,)), dma((2, 4)), dma((2,)), pltpu.SemaphoreType.REGULAR((3,)),
        ],
        compiler_params=pltpu.CompilerParams(collective_id=0, has_side_effects=True, vmem_limit_bytes=52000 * 2**10),
    )(
        *(
            pltpu.with_memory_space_constraint(array, pltpu.HBM)
            for array in (
                panels.transpose(1, 0, 2), out_grad.transpose(1, 0, 2),
                gate_weight[0], up_weight[0], down_weight[0],
            )
        )
    )
    grads = weight_updates(x_whole, dy_whole, packed)
    grad = grad.transpose(1, 0, 2)
    return (grad[None], *(g[None] for g in grads))


def fits_kernel(mesh, gate_weight, section_inputs):
    sizes = mesh.shape
    if (sizes["section"], sizes["row"], sizes["col"]) != (2, 4, 4):
        return False
    piece = gate_weight.shape[2] // (sizes["row"] * sizes["col"])
    local = section_inputs.shape[1] * section_inputs.shape[2] // sizes["col"]
    return piece % 128 == 0 and section_inputs.shape[3] % (256 * sizes["row"]) == 0 and local % 8 == 0 and (local * sizes["col"]) % 32 == 0


def solution(mesh):
    specs = dict(
        mesh=mesh,
        in_specs=(
            P("section", None, "col", "row"),
            P(None, "col", "row"),
            P("section", "row", "col"),
            P("section", "row", "col"),
            P("section", "col", "row"),
        ),
        out_specs=(
            P("section", None, "col", "row"),
            P("section", "row", "col"),
            P("section", "row", "col"),
            P("section", "col", "row"),
        ),
        check_vma=False,
    )

    def run(section_inputs, out_grad, gate_weight, up_weight, down_weight):
        body = fast_shards if fits_kernel(mesh, gate_weight, section_inputs) else shards
        return jax.shard_map(body, **specs)(section_inputs, out_grad, gate_weight, up_weight, down_weight)

    return run
```

```python
import jax
import jax.numpy as jnp
from jax import lax
from jax.experimental import pallas as pl
from jax.experimental.pallas import tpu as pltpu
from jax.sharding import PartitionSpec as P

CONTRACT_ROWS = (((0,), (0,)), ((), ()))
CONTRACT_COLS = (((1,), (1,)), ((), ()))


def passed_along(block, axis, distance):
    devices = range(lax.axis_size(axis))
    route = [(i - distance, i) for i in devices if i - distance in devices]
    return lax.ppermute(block, axis, route)


def spread_panel(panel):
    return lax.all_gather(panel, "col", axis=0, tiled=True)


def row_partials(make_terms, keep_rows):
    return lax.psum_scatter(
        make_terms(jnp.int32(0), keep_rows * lax.axis_size("row")).astype(jnp.bfloat16),
        "row",
        scatter_dimension=0,
        tiled=True,
    ).astype(jnp.float32)


def layer_backward(x_local, dy_local, w_both, w_down):
    hidden_width = w_down.shape[0]
    x_whole = spread_panel(x_local)
    dy_whole = spread_panel(dy_local)
    keep_rows = x_whole.shape[0] // lax.axis_size("row")

    def forward_terms(first_row, row_count):
        return jnp.dot(x_whole, w_both, preferred_element_type=jnp.float32)

    def backward_terms(first_row, row_count):
        return lax.dot_general(dy_whole, w_down, CONTRACT_COLS, preferred_element_type=jnp.float32)

    both_sums = row_partials(forward_terms, keep_rows)
    hidden_grad = row_partials(backward_terms, keep_rows)
    gate_sum = both_sums[:, :hidden_width]
    up_sum = both_sums[:, hidden_width:]
    sigmoid_gate = jax.nn.sigmoid(gate_sum)
    activated = gate_sum * sigmoid_gate
    slope = sigmoid_gate * (1.0 + gate_sum * (1.0 - sigmoid_gate))
    hidden = (activated * up_sum).astype(jnp.bfloat16)
    gate_grad = (hidden_grad * up_sum * slope).astype(jnp.bfloat16)
    up_grad = (hidden_grad * activated).astype(jnp.bfloat16)
    packed = jnp.concatenate([hidden, gate_grad, up_grad], axis=1)
    gathered = lax.all_gather(packed, "row", axis=0, tiled=True)
    hidden_whole = gathered[:, :hidden_width]
    both_grads = gathered[:, hidden_width:]
    branch_sum = lax.psum_scatter(
        lax.dot_general(
            both_grads, w_both, CONTRACT_COLS, preferred_element_type=jnp.float32
        ).astype(jnp.bfloat16),
        "col",
        scatter_dimension=0,
        tiled=True,
    ).astype(jnp.float32)
    input_grad = (dy_local.astype(jnp.float32) + branch_sum).astype(jnp.bfloat16)
    down_update = lax.dot_general(
        hidden_whole, dy_whole, CONTRACT_ROWS, preferred_element_type=jnp.float32
    )
    both_update = lax.dot_general(
        x_whole, both_grads, CONTRACT_ROWS, preferred_element_type=jnp.float32
    )
    return (input_grad, both_update, down_update)


def shards(section_inputs, out_grad, gate_weight, up_weight, down_weight):
    section_id = lax.axis_index("section")
    last_section = lax.axis_size("section") - 1
    is_last = section_id == last_section
    panels = section_inputs[0]
    w_both = jnp.concatenate([gate_weight[0], up_weight[0]], axis=1)
    w_down = down_weight[0]
    hidden_width = w_down.shape[0]
    micro_count = panels.shape[0]
    both_total = jnp.zeros(w_both.shape, jnp.float32)
    down_total = jnp.zeros(w_down.shape, jnp.float32)
    merged_shape = (micro_count * panels.shape[1], panels.shape[2])
    x_local = panels.reshape(merged_shape)
    top_grads = out_grad.reshape(merged_shape)
    received = jnp.zeros(merged_shape, jnp.bfloat16)
    merged_results = received
    for step_index in range(last_section + 1):
        is_active = section_id == last_section - step_index
        dy_local = jnp.where(is_last, top_grads, received)
        input_grad, both_update, down_update = layer_backward(x_local, dy_local, w_both, w_down)
        merged_results = jnp.where(is_active, input_grad, merged_results)
        both_total = both_total + jnp.where(is_active, both_update, 0.0)
        down_total = down_total + jnp.where(is_active, down_update, 0.0)
        if step_index < last_section:
            received = passed_along(input_grad, "section", -1)
    results = merged_results.reshape(panels.shape)
    return (
        results[None],
        both_total[:, :hidden_width][None],
        both_total[:, hidden_width:][None],
        down_total[None],
    )


ORDER = pl.DeviceIdType.MESH


def remote(src, dst, send_sem, recv_sem, target):
    return pltpu.make_async_remote_copy(
        src_ref=src, dst_ref=dst, send_sem=send_sem, recv_sem=recv_sem, device_id=target, device_id_type=ORDER
    )


def relay_kernel(
    x_ref, top_ref, gate_ref, up_ref, down_ref,
    x_whole, dy_whole, spread, result, ready,
    w_gate, w_up, w_down, turned, x_slots, dy_slots, stage, part_send, part_recv, gate_sum, up_sum, factors, middle,
    branch, branch_send, branch_recv,
    w_sem, in_sem, send_sem, x_recv_sem, dy_recv_sem, via_sem, pair_sem, last_part_sem,
    first_sem, second_sem, onward_sem, cross_sem, branch_recv_sem, go_sem,
):
    section = lax.axis_index("section")
    row = lax.axis_index("row")
    col = lax.axis_index("col")
    rows, width = part_send.shape[2], part_send.shape[3]
    local, micro = x_slots.shape[1:3]
    span = rows // 2
    group = local * micro
    block = x_slots.shape[3] // 2
    own = row
    is_top = section == 1
    is_bottom = section == 0

    def row_peer(d):
        hi, lo = row // 2, row % 2
        return ((hi + d // 2) % 2) * 2 + (lo + d % 2) % 2

    def ahead(d):
        return (col + d) % 4

    def behind(d):
        return (col + 4 - d) % 4

    def half(h):
        return pl.ds(h * span, span)

    def block_of(c):
        return pl.ds(pl.multiple_of(c * block, block), block)

    def piece_of(d):
        return pl.ds(pl.multiple_of(row_peer(d) * width, width), width)

    weights = ((gate_ref, w_gate), (up_ref, w_up), (down_ref, w_down))

    def weight_load(a):
        source, target = weights[a]
        size = target.shape[0] // 4
        for q in range(4):
            where = pl.ds(q * size, size)
            pltpu.make_async_copy(source.at[where, :], target.at[where, :], w_sem.at[a]).start()

    def weight_wait(a):
        source, target = weights[a]
        pltpu.make_async_copy(source, target, w_sem.at[a]).wait()

    def received(ref, sem):
        remote(ref, ref, send_sem.at[0], sem, (section, row, ahead(1))).wait_recv()

    def sent(ref, kind):
        remote(ref, ref, send_sem.at[kind], send_sem.at[kind], (section, row, ahead(1))).wait_send()

    def x_copy(d):
        return remote(x_slots.at[0], x_slots.at[d], send_sem.at[0], x_recv_sem.at[0], (section, row, ahead(d)))

    def dy_copy(d, c):
        return remote(
            dy_slots.at[c, 0], dy_slots.at[c, d], send_sem.at[1], dy_recv_sem.at[c], (section, row, ahead(d))
        )

    def pass_copy(d, c):
        return remote(result.at[:, :, block_of(c)], dy_slots.at[c, d], send_sem.at[6], dy_recv_sem.at[c], (0, row, ahead(d)))

    def part_copy(a, d, h, via, sem):
        place = (a, d, half(h), slice(None))
        return remote(
            part_send.at[place], part_recv.at[place], send_sem.at[2], sem, (section, row_peer(via), col)
        )

    def via_copy(a, h):
        return part_copy(a, 3, h, 1 + a, via_sem.at[a, h])

    def pair_copy(a, d, h):
        return part_copy(a, d, h, d, pair_sem.at[h])

    def last_part_copy(d, h):
        return part_copy(2, d, h, d, last_part_sem.at[h])

    def relay_sum(a, h):
        middle = 2 - a
        via_copy(a, h).wait_recv()
        total = part_send[a, middle, half(h), :].astype(jnp.float32) + part_recv[a, 3, half(h), :].astype(jnp.float32)
        part_send[a, middle, half(h), :] = total.astype(jnp.bfloat16)
        pair_copy(a, middle, h).start()

    def spread_copy(a, piece, d, h, sem):
        place = (a, piece, half(h), slice(None))
        return remote(spread.at[place], spread.at[place], send_sem.at[3], sem, (section, row_peer(d), col))

    def first_copy(a, h, piece=None):
        d = (1 + h, 1, 2)[a]
        return spread_copy(a, own if piece is None else row_peer(d), d, h, first_sem.at[a, h])

    def second_copy(a, h, piece=None):
        d = (2 - h, 2, 1)[a]
        return spread_copy(a, own if piece is None else row_peer(d), d, h, second_sem.at[a, h if a == 0 else 0])

    def onward_copy(a, h):
        d = (1 + h, 1, 2)[a]
        return remote(
            spread.at[a, row_peer(d), half(h), :], spread.at[a, row_peer(d), half(h), :],
            send_sem.at[4], onward_sem.at[min(a, 1)], (section, row_peer(3 - d), col),
        )

    def spread_grads(h):
        for a in (1, 2):
            first_copy(a, h).start()
        for a in (2, 1):
            second_copy(a, h).start()

    def relay_grads(h):
        for a in (1, 2):
            first_copy(a, h, 1).wait_recv()
            onward_copy(a, h).start()

    def spread_hidden():
        for h in range(2):
            first_copy(0, h).start()
        for h in (1, 0):
            second_copy(0, h).start()

    def relay_hidden():
        for h in range(2):
            first_copy(0, h, 1).wait_recv()
            onward_copy(0, h).start()

    def cross_copy(step, i, h):
        source, target = ((part_send.at[2], part_recv.at[2]), (middle.at[0], middle.at[1]))[step]
        return remote(
            source.at[i, half(h), :], target.at[i, half(h), :],
            send_sem.at[7 + step], cross_sem.at[step, i], (section, row_peer(1 + (step + h) % 2), col),
        )

    def branch_copy(d, c):
        return remote(
            branch_send.at[c, d], branch_recv.at[c, d], send_sem.at[5], branch_recv_sem.at[c], (section, row, behind(d))
        )

    def ready_step(j, carry):
        tall = ready.shape[1]
        where = pl.ds(pl.multiple_of(j * tall, tall), tall)
        for p in range(4):
            ready[j, :, p * width:(p + 1) * width] = lax.dot_general(
                x_whole[:, where], spread[1, p], CONTRACT_ROWS, preferred_element_type=jnp.float32
            )
        return carry

    def merge(slots):
        for d in range(4):
            for t in range(local):
                first = d * group + t * micro
                stage[first:first + micro, :slots.shape[3]] = slots[d, t].astype(jnp.float32)

    x_load = pltpu.make_async_copy(x_ref, x_slots.at[0], in_sem.at[0])

    def top_load(c):
        return pltpu.make_async_copy(top_ref.at[:, :, block_of(c)], dy_slots.at[c, 0], in_sem.at[1 + c])

    x_load.start()

    @pl.when(is_top)
    def _():
        for c in range(2):
            top_load(c).start()

    barrier = pltpu.get_barrier_semaphore()
    greeted = [(section, row, ahead(d)) for d in (1, 2, 3)]
    greeted += [(section, row_peer(d), col) for d in (1, 2, 3)]
    greeted += [(1 - section, row, ahead(d)) for d in range(4)]
    for device in greeted:
        pl.semaphore_signal(barrier, inc=1, device_id=device, device_id_type=ORDER)
    x_load.wait()

    @pl.when(is_top)
    def _():
        for c in range(2):
            top_load(c).wait()

    for a in range(3):
        weight_load(a)

    pl.semaphore_wait(barrier, len(greeted))

    def partner_go(which):
        pl.semaphore_signal(
            go_sem.at[which], inc=1, device_id=(1 - section, row, col), device_id_type=ORDER
        )

    @pl.when(is_bottom)
    def _():
        pl.semaphore_wait(go_sem.at[0], 1)

    for d in (2, 1, 3):
        x_copy(d).start()

    @pl.when(is_top)
    def _():
        for c in range(2):
            for d in (2, 1, 3):
                dy_copy(d, c).start()

    received(x_slots.at[pl.ds(1, 3)], x_recv_sem.at[0])
    merge(x_slots)

    @pl.when(is_top)
    def _():
        partner_go(0)

    x_whole[...] = stage[...].astype(jnp.bfloat16)
    for a in range(2):
        weight_wait(a)

    def forward_step(i, carry):
        d = 3 - i
        for a, weight in enumerate((w_gate, w_up)):
            part_send[a, d] = jnp.dot(
                x_whole[...], weight[:, piece_of(d)], preferred_element_type=jnp.float32
            ).astype(jnp.bfloat16)

            @pl.when(jnp.logical_and(is_top, d == 3))
            def _():
                for h in range(2):
                    via_copy(a, h).start()

            @pl.when(jnp.logical_and(is_top, d == 1 + a))
            def _():
                for h in range(2):
                    pair_copy(a, 1 + a, h).start()
        return carry

    lax.fori_loop(0, 4, forward_step, 0)

    def summed(a, where):
        total = part_send[a, 0, where, :].astype(jnp.float32)
        for d in range(1, 4 if a == 2 else 3):
            total = total + part_recv[a, d, where, :].astype(jnp.float32)
        return total

    def rows_of(i):
        return pl.ds(pl.multiple_of(i * 16, 16), 16)

    def sum_step(i, carry):
        where = rows_of(i)
        spread[1, own, where, :] = summed(0, where).astype(jnp.bfloat16)
        spread[2, own, where, :] = summed(1, where).astype(jnp.bfloat16)
        return carry

    def hidden_step(i, carry):
        where = rows_of(i)
        gate, up = summed(0, where), summed(1, where)
        gate_sum[where, :] = gate
        up_sum[where, :] = up
        spread[0, own, where, :] = (gate * jax.nn.sigmoid(gate) * up).astype(jnp.bfloat16)
        return carry

    def factor_rows(first, count):
        def step(k, carry):
            d = row_peer(first + k // (2 * steps))
            where = rows_of(k % (2 * steps))
            gate = spread[1, d, where, :].astype(jnp.float32)
            up = spread[2, d, where, :].astype(jnp.float32)
            sigmoid_gate = jax.nn.sigmoid(gate)
            activated = gate * sigmoid_gate
            slope = sigmoid_gate * (1.0 + gate * (1.0 - sigmoid_gate))
            spread[0, d, where, :] = (activated * up).astype(jnp.bfloat16)
            factors[0, d, where, :] = up * slope
            factors[1, d, where, :] = activated
            return carry

        lax.fori_loop(0, count * 2 * steps, step, 0)

    def grad_step(i, carry):
        where = rows_of(i)
        hidden_grad = summed(2, where)
        gate, up = gate_sum[where, :], up_sum[where, :]
        sigmoid_gate = jax.nn.sigmoid(gate)
        slope = sigmoid_gate * (1.0 + gate * (1.0 - sigmoid_gate))
        spread[1, own, where, :] = (hidden_grad * up * slope).astype(jnp.bfloat16)
        spread[2, own, where, :] = (hidden_grad * (gate * sigmoid_gate)).astype(jnp.bfloat16)
        return carry

    steps = span // 16

    def hidden_rows(h):
        received(part_recv.at[pl.ds(0, 2), pl.ds(1, 2), half(h), :], pair_sem.at[h])
        lax.fori_loop(h * steps, (h + 1) * steps, hidden_step, 0)

    def grad_rows(h):
        received(part_recv.at[2, pl.ds(1, 3), half(h), :], last_part_sem.at[h])
        lax.fori_loop(h * steps, (h + 1) * steps, grad_step, 0)
        spread_grads(h)

    @pl.when(is_bottom)
    def _():
        strip = 256 if turned.shape[1] % 256 == 0 else 128

        def turn(k, inner):
            cols = pl.ds(pl.multiple_of(k * strip, strip), strip)
            for a, weight in enumerate((w_gate, w_up)):
                turned[a, cols, :] = weight[:, cols].T
            return inner

        lax.fori_loop(0, turned.shape[1] // strip, turn, 0)
        pl.semaphore_wait(go_sem.at[1], 1)
        for h in range(2):
            for a in range(2):
                via_copy(a, h).start()
        for h in range(2):
            for a in range(2):
                pair_copy(a, 1 + a, h).start()

    for a in range(2):
        relay_sum(a, 0)

    @pl.when(is_bottom)
    def _():
        for a in range(2):
            relay_sum(a, 1)
        for h in range(2):
            received(part_recv.at[pl.ds(0, 2), pl.ds(1, 2), half(h), :], pair_sem.at[h])
            lax.fori_loop(h * steps, (h + 1) * steps, sum_step, 0)
            spread_grads(h)
        relay_grads(0)

    def merge_block(c):
        @pl.when(is_top)
        def _():
            received(dy_slots.at[c, pl.ds(1, 3)], dy_recv_sem.at[c])

        @pl.when(is_bottom)
        def _():
            received(dy_slots.at[c], dy_recv_sem.at[c])

        merge(dy_slots.at[c])
        dy_whole[:, c * block:(c + 1) * block] = stage[:, :block].astype(jnp.bfloat16)

    weight_wait(2)

    for c in range(2):
        merge_block(c)

    def grad_terms_step(i, carry):
        d = section * (3 - i) + (1 - section) * i
        owner = section * row_peer(d) + (1 - section) * i
        piece = pl.ds(pl.multiple_of(owner * width, width), width)
        part_send[2, d] = lax.dot_general(
            dy_whole[...], w_down[piece, :], CONTRACT_COLS, preferred_element_type=jnp.float32
        ).astype(jnp.bfloat16)

        @pl.when(is_bottom)
        def _():
            for h in range(2):
                cross_copy(0, i, h).start()

        @pl.when(jnp.logical_and(is_top, d > 0))
        def _():
            last_part_copy(d, 0).start()

        @pl.when(jnp.logical_and(is_top, i == 1))
        def _():
            for a in range(2):
                relay_sum(a, 1)
        return carry

    lax.fori_loop(0, 4, grad_terms_step, 0)

    @pl.when(is_top)
    def _():
        for d in (3, 2, 1):
            last_part_copy(d, 1).start()
        for h in range(2):
            hidden_rows(h)
        for h in range(2):
            grad_rows(h)

    def send_branch(c):
        for d in (2, 3, 1):
            first = d * group
            branch_send[c, d] = branch[first:first + group, c * block:(c + 1) * block].astype(jnp.bfloat16)
            branch_copy(d, c).start()

    def branch_terms(d, cols):
        return lax.dot_general(
            spread[1, row_peer(d)], w_gate[cols, piece_of(d)], CONTRACT_COLS, preferred_element_type=jnp.float32
        ) + lax.dot_general(
            spread[2, row_peer(d)], w_up[cols, piece_of(d)], CONTRACT_COLS, preferred_element_type=jnp.float32
        )

    def branch_step(d, carry):
        @pl.when(d == 1)
        def _():
            relay_grads(0)
            partner_go(1)
            relay_grads(1)
            received(spread.at[2, row_peer(1)], second_sem.at[2, 0])

        @pl.when(d == 2)
        def _():
            received(spread.at[1, row_peer(2)], second_sem.at[1, 0])

        term = branch_terms(d, slice(None))

        @pl.when(d == 0)
        def _():
            branch[...] = term

        @pl.when(d > 0)
        def _():
            branch[...] += term
        return carry

    def last_branch_step(c, carry):
        @pl.when(c == 1)
        def _():
            send_branch(0)

        branch[:, block_of(c)] += branch_terms(3, block_of(c))
        return carry

    def finish_hidden():
        for h in range(2):
            second_copy(0, h, 1).wait_recv()
        received(spread.at[0, row_peer(3)], onward_sem.at[0])

    @pl.when(is_top)
    def _():
        lax.fori_loop(0, 3, branch_step, 0)
        received(spread.at[pl.ds(1, 2), row_peer(3)], onward_sem.at[1])
        lax.fori_loop(0, 2, last_branch_step, 0)

    def cross_sum(i):
        received(part_recv.at[2, i], cross_sem.at[0, i])
        total = part_send[2, i].astype(jnp.float32) + part_recv[2, i].astype(jnp.float32)
        middle[0, i] = total.astype(jnp.bfloat16)
        for h in range(2):
            cross_copy(1, i, h).start()

    def cross_grads(i):
        received(middle.at[1, i], cross_sem.at[1, i])

        def grads(k, carry):
            where = rows_of(k)
            hidden_grad = middle[0, i, where, :].astype(jnp.float32) + middle[1, i, where, :].astype(jnp.float32)
            for a in range(2):
                spread[1 + a, i, where, :] = (hidden_grad * factors[a, i, where, :]).astype(jnp.bfloat16)
            return carry

        lax.fori_loop(0, 2 * steps, grads, 0)

    def turned_terms(i, cols):
        piece = pl.ds(i * width if isinstance(i, int) else pl.multiple_of(i * width, width), width)
        term = jnp.dot(spread[1, i], turned[0, piece, cols], preferred_element_type=jnp.float32)
        return term + jnp.dot(spread[2, i], turned[1, piece, cols], preferred_element_type=jnp.float32)

    def cross_step(i, carry):
        cross_grads(i)
        term = turned_terms(i, slice(None))

        @pl.when(i == 0)
        def _():
            branch[...] = term

        @pl.when(i > 0)
        def _():
            branch[...] += term
        return carry

    def last_cross_step(c, carry):
        @pl.when(c == 1)
        def _():
            send_branch(0)

        branch[:, block_of(c)] += turned_terms(3, block_of(c))
        return carry

    @pl.when(is_bottom)
    def _():
        relay_grads(1)
        received(spread.at[2, row_peer(1)], second_sem.at[2, 0])
        received(spread.at[1, row_peer(2)], second_sem.at[1, 0])
        factor_rows(0, 3)
        for i in range(4):
            cross_sum(i)
        received(spread.at[pl.ds(1, 2), row_peer(3)], onward_sem.at[1])
        factor_rows(3, 1)
        sent(spread.at[pl.ds(1, 2), pl.ds(1, 2)], 3)
        sent(spread.at[pl.ds(1, 2), 3], 4)
        lax.fori_loop(0, 3, cross_step, 0)
        cross_grads(3)
        lax.fori_loop(0, 2, last_cross_step, 0)

    send_branch(1)

    @pl.when(is_top)
    def _():
        spread_hidden()

    @pl.when(is_bottom)
    def _():
        lax.fori_loop(0, ready.shape[0], ready_step, 0)

    for c in range(2):
        cols = slice(c * block, (c + 1) * block)
        total = dy_whole[:group, cols].astype(jnp.float32) + branch[:group, cols]
        received(branch_recv.at[c, pl.ds(1, 3)], branch_recv_sem.at[c])
        for d in (1, 2, 3):
            total = total + branch_recv[c, d].astype(jnp.float32)
        stage[:group, :block] = total
        for t in range(local):
            result[t, :, cols] = stage[t * micro:(t + 1) * micro, :block].astype(jnp.bfloat16)

        @pl.when(is_top)
        def _():
            for d in (2, 3, 1, 0):
                pass_copy(d, c).start()

    @pl.when(is_top)
    def _():
        relay_hidden()
        lax.fori_loop(0, ready.shape[0], ready_step, 0)
        finish_hidden()
        sent(dy_slots.at[:, pl.ds(1, 3)], 1)
        sent(dy_slots, 6)
        sent(part_send.at[:, pl.ds(1, 3)], 2)
        sent(spread.at[:, pl.ds(1, 2)], 3)
        sent(spread.at[:, 3], 4)

    @pl.when(is_bottom)
    def _():
        sent(part_send.at[pl.ds(0, 2), pl.ds(1, 3)], 2)
        sent(part_send.at[2], 7)
        sent(middle.at[0], 8)

    sent(branch_send.at[:, pl.ds(1, 3)], 5)
    sent(x_slots.at[pl.ds(1, 3)], 0)

def update_kernel(x_ref, dy_ref, packed_ref, ready_ref, gate_out, up_out, down_out, wide_tiles, down_tiles, sem, ready_sem):
    pieces, rows, piece = packed_ref.shape[1:]
    tall = wide_tiles.shape[1]
    made, blocks = ready_ref.shape[0], x_ref.shape[1] // tall

    def where_of(j):
        return pl.ds(j * tall if isinstance(j, int) else pl.multiple_of(j * tall, tall), tall)

    ready_copies = [
        pltpu.make_async_copy(ready_ref.at[j], gate_out.at[where_of(j), :], ready_sem.at[j]) for j in range(made)
    ]
    for copy in ready_copies:
        copy.start()

    def wide_step(k, carry):
        a = (k + made) // blocks
        where = where_of((k + made) % blocks)
        for p in range(pieces):
            wide_tiles[k, :, p * piece:(p + 1) * piece] = lax.dot_general(
                x_ref[:, where], packed_ref[1 + a, p], CONTRACT_ROWS, preferred_element_type=jnp.float32
            )
        for b, target in enumerate((gate_out, up_out)):
            @pl.when(a == b)
            def _():
                pltpu.make_async_copy(wide_tiles.at[k], target.at[where, :], sem.at[0]).start()
        return carry

    lax.fori_loop(0, wide_tiles.shape[0], wide_step, 0)

    def down_step(p, carry):
        where = pl.ds(pl.multiple_of(p * piece, piece), piece)
        down_tiles[p] = lax.dot_general(
            packed_ref[0, p], dy_ref[...], CONTRACT_ROWS, preferred_element_type=jnp.float32
        )
        pltpu.make_async_copy(down_tiles.at[p], down_out.at[where, :], sem.at[1]).start()
        return carry

    lax.fori_loop(0, pieces, down_step, 0)
    for copy in ready_copies:
        copy.wait()
    for a, tiles in enumerate((wide_tiles, down_tiles)):
        pltpu.make_async_copy(tiles, tiles, sem.at[a]).wait()


def weight_updates(x_whole, dy_whole, packed, ready):
    rows, width = x_whole.shape
    pieces, piece = packed.shape[1], packed.shape[3]
    hidden_width = pieces * piece
    made, tall = ready.shape[:2]
    f32 = jnp.float32
    vmem = pl.BlockSpec(memory_space=pltpu.VMEM)
    hbm = pl.BlockSpec(memory_space=pltpu.HBM)
    return pl.pallas_call(
        update_kernel,
        out_shape=(
            jax.ShapeDtypeStruct((width, hidden_width), f32),
            jax.ShapeDtypeStruct((width, hidden_width), f32),
            jax.ShapeDtypeStruct((hidden_width, width), f32),
        ),
        in_specs=[vmem, vmem, vmem, vmem],
        out_specs=(hbm, hbm, hbm),
        scratch_shapes=[
            pltpu.VMEM((2 * width // tall - made, tall, hidden_width), f32),
            pltpu.VMEM((pieces, piece, width), f32),
            pltpu.SemaphoreType.DMA((2,)),
            pltpu.SemaphoreType.DMA((made,)),
        ],
        compiler_params=pltpu.CompilerParams(vmem_limit_bytes=44 * 2**20),
        cost_estimate=pl.CostEstimate(
            flops=6 * rows * width * hidden_width,
            bytes_accessed=12 * width * hidden_width + 2 * rows * (2 * width + 3 * hidden_width),
            transcendentals=0,
        ),
    )(x_whole, dy_whole, packed, ready)


def fast_shards(section_inputs, out_grad, gate_weight, up_weight, down_weight):
    panels = section_inputs[0]
    micro, local, width = panels.shape
    group = micro * local
    held = (local, micro, width)
    rows = group * lax.axis_size("col")
    hidden_width = gate_weight.shape[2]
    piece = hidden_width // lax.axis_size("row")
    hbm = pl.BlockSpec(memory_space=pltpu.HBM)
    vmem = pl.BlockSpec(memory_space=pltpu.VMEM)
    bf16, f32 = jnp.bfloat16, jnp.float32
    dma = pltpu.SemaphoreType.DMA
    block = width // 2
    tall = 256 if width % 256 == 0 else 128
    x_whole, dy_whole, packed, grad, ready = pl.pallas_call(
        relay_kernel,
        out_shape=(
            jax.ShapeDtypeStruct((rows, width), bf16),
            jax.ShapeDtypeStruct((rows, width), bf16),
            jax.ShapeDtypeStruct((3, 4, rows, piece), bf16),
            jax.ShapeDtypeStruct(held, bf16),
            jax.ShapeDtypeStruct((1, tall, hidden_width), f32),
        ),
        in_specs=[hbm] * 5,
        out_specs=(vmem,) * 5,
        scratch_shapes=[
            pltpu.VMEM((width, hidden_width), bf16),
            pltpu.VMEM((width, hidden_width), bf16),
            pltpu.VMEM((hidden_width, width), bf16),
            pltpu.VMEM((2, hidden_width, width), bf16),
            pltpu.VMEM((4, *held), bf16),
            pltpu.VMEM((2, 4, local, micro, block), bf16),
            pltpu.VMEM((rows, width), f32),
            pltpu.VMEM((3, 4, rows, piece), bf16),
            pltpu.VMEM((3, 4, rows, piece), bf16),
            pltpu.VMEM((rows, piece), f32),
            pltpu.VMEM((rows, piece), f32),
            pltpu.VMEM((2, 4, rows, piece), f32),
            pltpu.VMEM((2, 4, rows, piece), bf16),
            pltpu.VMEM((rows, width), f32),
            pltpu.VMEM((2, 4, group, block), bf16),
            pltpu.VMEM((2, 4, group, block), bf16),
            dma((3,)), dma((3,)), dma((9,)), dma((1,)), dma((2,)), dma((2, 2)), dma((2,)), dma((2,)),
            dma((3, 2)), dma((3, 2)), dma((2,)), dma((2, 4)), dma((2,)), pltpu.SemaphoreType.REGULAR((2,)),
        ],
        compiler_params=pltpu.CompilerParams(collective_id=0, has_side_effects=True, vmem_limit_bytes=46800 * 2**10),
    )(
        *(
            pltpu.with_memory_space_constraint(array, pltpu.HBM)
            for array in (
                panels.transpose(1, 0, 2), out_grad.transpose(1, 0, 2),
                gate_weight[0], up_weight[0], down_weight[0],
            )
        )
    )
    grads = weight_updates(x_whole, dy_whole, packed, ready)
    grad = grad.transpose(1, 0, 2)
    return (grad[None], *(g[None] for g in grads))


def fits_kernel(mesh, gate_weight, section_inputs):
    sizes = mesh.shape
    if (sizes["section"], sizes["row"], sizes["col"]) != (2, 4, 4):
        return False
    piece = gate_weight.shape[2] // (sizes["row"] * sizes["col"])
    local = section_inputs.shape[1] * section_inputs.shape[2] // sizes["col"]
    return piece % 128 == 0 and section_inputs.shape[3] % (256 * sizes["row"]) == 0 and local % 8 == 0 and (local * sizes["col"]) % 32 == 0


def solution(mesh):
    specs = dict(
        mesh=mesh,
        in_specs=(
            P("section", None, "col", "row"),
            P(None, "col", "row"),
            P("section", "row", "col"),
            P("section", "row", "col"),
            P("section", "col", "row"),
        ),
        out_specs=(
            P("section", None, "col", "row"),
            P("section", "row", "col"),
            P("section", "row", "col"),
            P("section", "col", "row"),
        ),
        check_vma=False,
    )

    def run(section_inputs, out_grad, gate_weight, up_weight, down_weight):
        body = fast_shards if fits_kernel(mesh, gate_weight, section_inputs) else shards
        return jax.shard_map(body, **specs)(section_inputs, out_grad, gate_weight, up_weight, down_weight)

    return run
```

```python
import jax
import jax.numpy as jnp
from jax import lax
from jax.experimental import pallas as pl
from jax.experimental.pallas import tpu as pltpu
from jax.sharding import PartitionSpec as P

CONTRACT_ROWS = (((0,), (0,)), ((), ()))
CONTRACT_COLS = (((1,), (1,)), ((), ()))


def passed_along(block, axis, distance):
    devices = range(lax.axis_size(axis))
    route = [(i - distance, i) for i in devices if i - distance in devices]
    return lax.ppermute(block, axis, route)


def spread_panel(panel):
    return lax.all_gather(panel, "col", axis=0, tiled=True)


def row_partials(make_terms, keep_rows):
    return lax.psum_scatter(
        make_terms(jnp.int32(0), keep_rows * lax.axis_size("row")).astype(jnp.bfloat16),
        "row",
        scatter_dimension=0,
        tiled=True,
    ).astype(jnp.float32)


def layer_backward(x_local, dy_local, w_both, w_down):
    hidden_width = w_down.shape[0]
    x_whole = spread_panel(x_local)
    dy_whole = spread_panel(dy_local)
    keep_rows = x_whole.shape[0] // lax.axis_size("row")

    def forward_terms(first_row, row_count):
        return jnp.dot(x_whole, w_both, preferred_element_type=jnp.float32)

    def backward_terms(first_row, row_count):
        return lax.dot_general(dy_whole, w_down, CONTRACT_COLS, preferred_element_type=jnp.float32)

    both_sums = row_partials(forward_terms, keep_rows)
    hidden_grad = row_partials(backward_terms, keep_rows)
    gate_sum = both_sums[:, :hidden_width]
    up_sum = both_sums[:, hidden_width:]
    sigmoid_gate = jax.nn.sigmoid(gate_sum)
    activated = gate_sum * sigmoid_gate
    slope = sigmoid_gate * (1.0 + gate_sum * (1.0 - sigmoid_gate))
    hidden = (activated * up_sum).astype(jnp.bfloat16)
    gate_grad = (hidden_grad * up_sum * slope).astype(jnp.bfloat16)
    up_grad = (hidden_grad * activated).astype(jnp.bfloat16)
    packed = jnp.concatenate([hidden, gate_grad, up_grad], axis=1)
    gathered = lax.all_gather(packed, "row", axis=0, tiled=True)
    hidden_whole = gathered[:, :hidden_width]
    both_grads = gathered[:, hidden_width:]
    branch_sum = lax.psum_scatter(
        lax.dot_general(
            both_grads, w_both, CONTRACT_COLS, preferred_element_type=jnp.float32
        ).astype(jnp.bfloat16),
        "col",
        scatter_dimension=0,
        tiled=True,
    ).astype(jnp.float32)
    input_grad = (dy_local.astype(jnp.float32) + branch_sum).astype(jnp.bfloat16)
    down_update = lax.dot_general(
        hidden_whole, dy_whole, CONTRACT_ROWS, preferred_element_type=jnp.float32
    )
    both_update = lax.dot_general(
        x_whole, both_grads, CONTRACT_ROWS, preferred_element_type=jnp.float32
    )
    return (input_grad, both_update, down_update)


def shards(section_inputs, out_grad, gate_weight, up_weight, down_weight):
    section_id = lax.axis_index("section")
    last_section = lax.axis_size("section") - 1
    is_last = section_id == last_section
    panels = section_inputs[0]
    w_both = jnp.concatenate([gate_weight[0], up_weight[0]], axis=1)
    w_down = down_weight[0]
    hidden_width = w_down.shape[0]
    micro_count = panels.shape[0]
    both_total = jnp.zeros(w_both.shape, jnp.float32)
    down_total = jnp.zeros(w_down.shape, jnp.float32)
    merged_shape = (micro_count * panels.shape[1], panels.shape[2])
    x_local = panels.reshape(merged_shape)
    top_grads = out_grad.reshape(merged_shape)
    received = jnp.zeros(merged_shape, jnp.bfloat16)
    merged_results = received
    for step_index in range(last_section + 1):
        is_active = section_id == last_section - step_index
        dy_local = jnp.where(is_last, top_grads, received)
        input_grad, both_update, down_update = layer_backward(x_local, dy_local, w_both, w_down)
        merged_results = jnp.where(is_active, input_grad, merged_results)
        both_total = both_total + jnp.where(is_active, both_update, 0.0)
        down_total = down_total + jnp.where(is_active, down_update, 0.0)
        if step_index < last_section:
            received = passed_along(input_grad, "section", -1)
    results = merged_results.reshape(panels.shape)
    return (
        results[None],
        both_total[:, :hidden_width][None],
        both_total[:, hidden_width:][None],
        down_total[None],
    )


ORDER = pl.DeviceIdType.MESH


def remote(src, dst, send_sem, recv_sem, target):
    return pltpu.make_async_remote_copy(
        src_ref=src, dst_ref=dst, send_sem=send_sem, recv_sem=recv_sem, device_id=target, device_id_type=ORDER
    )


def relay_kernel(
    x_ref, top_ref, gate_ref, up_ref, down_ref,
    x_whole, dy_whole, spread, result, ready,
    w_gate, w_up, w_down, turned, x_slots, dy_slots, stage, part_send, part_recv, gate_sum, up_sum, factors, middle,
    branch, branch_send, branch_recv,
    w_sem, in_sem, send_sem, x_recv_sem, dy_recv_sem, via_sem, pair_sem, last_part_sem,
    first_sem, second_sem, onward_sem, cross_sem, branch_recv_sem, go_sem,
):
    section = lax.axis_index("section")
    row = lax.axis_index("row")
    col = lax.axis_index("col")
    rows, width = part_send.shape[2], part_send.shape[3]
    local, micro = x_slots.shape[1:3]
    span = rows // 2
    group = local * micro
    block = x_slots.shape[3] // 2
    own = row
    is_top = section == 1
    is_bottom = section == 0

    def row_peer(d):
        hi, lo = row // 2, row % 2
        return ((hi + d // 2) % 2) * 2 + (lo + d % 2) % 2

    def ahead(d):
        return (col + d) % 4

    def behind(d):
        return (col + 4 - d) % 4

    def half(h):
        return pl.ds(h * span, span)

    def block_of(c):
        return pl.ds(pl.multiple_of(c * block, block), block)

    def piece_of(d):
        return pl.ds(pl.multiple_of(row_peer(d) * width, width), width)

    weights = ((gate_ref, w_gate), (up_ref, w_up), (down_ref, w_down))

    def weight_load(a):
        source, target = weights[a]
        size = target.shape[0] // 4
        for q in range(4):
            where = pl.ds(q * size, size)
            pltpu.make_async_copy(source.at[where, :], target.at[where, :], w_sem.at[a]).start()

    def weight_wait(a):
        source, target = weights[a]
        pltpu.make_async_copy(source, target, w_sem.at[a]).wait()

    def received(ref, sem):
        remote(ref, ref, send_sem.at[0], sem, (section, row, ahead(1))).wait_recv()

    def sent(ref, kind):
        remote(ref, ref, send_sem.at[kind], send_sem.at[kind], (section, row, ahead(1))).wait_send()

    def x_copy(d):
        return remote(x_slots.at[0], x_slots.at[d], send_sem.at[0], x_recv_sem.at[0], (section, row, ahead(d)))

    def dy_copy(d, c):
        return remote(
            dy_slots.at[c, 0], dy_slots.at[c, d], send_sem.at[1], dy_recv_sem.at[c], (section, row, ahead(d))
        )

    def pass_copy(d, c):
        return remote(result.at[:, :, block_of(c)], dy_slots.at[c, d], send_sem.at[6], dy_recv_sem.at[c], (0, row, ahead(d)))

    def part_copy(a, d, h, via, sem):
        place = (a, d, half(h), slice(None))
        return remote(
            part_send.at[place], part_recv.at[place], send_sem.at[2], sem, (section, row_peer(via), col)
        )

    def via_copy(a, h):
        return part_copy(a, 3, h, 1 + a, via_sem.at[a, h])

    def pair_copy(a, d, h):
        return part_copy(a, d, h, d, pair_sem.at[h])

    def last_part_copy(d, h):
        return part_copy(2, d, h, d, last_part_sem.at[h])

    def relay_sum(a, h):
        middle = 2 - a
        via_copy(a, h).wait_recv()
        total = part_send[a, middle, half(h), :].astype(jnp.float32) + part_recv[a, 3, half(h), :].astype(jnp.float32)
        part_send[a, middle, half(h), :] = total.astype(jnp.bfloat16)
        pair_copy(a, middle, h).start()

    def spread_copy(a, piece, d, h, sem):
        place = (a, piece, half(h), slice(None))
        return remote(spread.at[place], spread.at[place], send_sem.at[3], sem, (section, row_peer(d), col))

    def first_copy(a, h, piece=None):
        d = (1 + h, 1, 2)[a]
        return spread_copy(a, own if piece is None else row_peer(d), d, h, first_sem.at[a, h])

    def second_copy(a, h, piece=None):
        d = (2 - h, 2, 1)[a]
        return spread_copy(a, own if piece is None else row_peer(d), d, h, second_sem.at[a, h if a == 0 else 0])

    def onward_copy(a, h):
        d = (1 + h, 1, 2)[a]
        return remote(
            spread.at[a, row_peer(d), half(h), :], spread.at[a, row_peer(d), half(h), :],
            send_sem.at[4], onward_sem.at[min(a, 1)], (section, row_peer(3 - d), col),
        )

    def spread_grads(h):
        for a in (1, 2):
            first_copy(a, h).start()
        for a in (2, 1):
            second_copy(a, h).start()

    def relay_grads(h):
        for a in (1, 2):
            first_copy(a, h, 1).wait_recv()
            onward_copy(a, h).start()

    def spread_hidden():
        for h in range(2):
            first_copy(0, h).start()
        for h in (1, 0):
            second_copy(0, h).start()

    def relay_hidden():
        for h in range(2):
            first_copy(0, h, 1).wait_recv()
            onward_copy(0, h).start()

    def cross_copy(step, i, h):
        source, target = ((part_send.at[2], part_recv.at[2]), (middle.at[0], middle.at[1]))[step]
        return remote(
            source.at[i, half(h), :], target.at[i, half(h), :],
            send_sem.at[7 + step], cross_sem.at[step, i], (section, row_peer(1 + (step + h) % 2), col),
        )

    def branch_copy(d, c):
        return remote(
            branch_send.at[c, d], branch_recv.at[c, d], send_sem.at[5], branch_recv_sem.at[c], (section, row, behind(d))
        )

    def ready_step(j, carry):
        tall = ready.shape[1]
        where = pl.ds(pl.multiple_of(j * tall, tall), tall)
        for p in range(4):
            ready[j, :, p * width:(p + 1) * width] = lax.dot_general(
                x_whole[:, where], spread[1, p], CONTRACT_ROWS, preferred_element_type=jnp.float32
            )
        return carry

    def merge(slots):
        for d in range(4):
            for t in range(local):
                first = d * group + t * micro
                stage[first:first + micro, :slots.shape[3]] = slots[d, t].astype(jnp.float32)

    x_load = pltpu.make_async_copy(x_ref, x_slots.at[0], in_sem.at[0])

    def top_load(c):
        return pltpu.make_async_copy(top_ref.at[:, :, block_of(c)], dy_slots.at[c, 0], in_sem.at[1 + c])

    x_load.start()

    @pl.when(is_top)
    def _():
        for c in range(2):
            top_load(c).start()

    barrier = pltpu.get_barrier_semaphore()
    greeted = [(section, row, ahead(d)) for d in (1, 2, 3)]
    greeted += [(section, row_peer(d), col) for d in (1, 2, 3)]
    greeted += [(1 - section, row, ahead(d)) for d in range(4)]
    for device in greeted:
        pl.semaphore_signal(barrier, inc=1, device_id=device, device_id_type=ORDER)
    x_load.wait()

    @pl.when(is_top)
    def _():
        for c in range(2):
            top_load(c).wait()

    for a in range(3):
        weight_load(a)

    pl.semaphore_wait(barrier, len(greeted))

    def partner_go(which):
        pl.semaphore_signal(
            go_sem.at[which], inc=1, device_id=(1 - section, row, col), device_id_type=ORDER
        )

    @pl.when(is_bottom)
    def _():
        pl.semaphore_wait(go_sem.at[0], 1)

    for d in (2, 1, 3):
        x_copy(d).start()

    @pl.when(is_top)
    def _():
        for c in range(2):
            for d in (2, 1, 3):
                dy_copy(d, c).start()

    received(x_slots.at[pl.ds(1, 3)], x_recv_sem.at[0])
    merge(x_slots)

    @pl.when(is_top)
    def _():
        partner_go(0)

    x_whole[...] = stage[...].astype(jnp.bfloat16)
    for a in range(2):
        weight_wait(a)

    def forward_step(i, carry):
        d = 3 - i
        for a, weight in enumerate((w_gate, w_up)):
            part_send[a, d] = jnp.dot(
                x_whole[...], weight[:, piece_of(d)], preferred_element_type=jnp.float32
            ).astype(jnp.bfloat16)

            @pl.when(jnp.logical_and(is_top, d == 3))
            def _():
                for h in range(2):
                    via_copy(a, h).start()

            @pl.when(jnp.logical_and(is_top, d == 1 + a))
            def _():
                for h in range(2):
                    pair_copy(a, 1 + a, h).start()
        return carry

    lax.fori_loop(0, 4, forward_step, 0)

    def summed(a, where):
        total = part_send[a, 0, where, :].astype(jnp.float32)
        for d in range(1, 4 if a == 2 else 3):
            total = total + part_recv[a, d, where, :].astype(jnp.float32)
        return total

    def rows_of(i):
        return pl.ds(pl.multiple_of(i * 16, 16), 16)

    def sum_step(i, carry):
        where = rows_of(i)
        spread[1, own, where, :] = summed(0, where).astype(jnp.bfloat16)
        spread[2, own, where, :] = summed(1, where).astype(jnp.bfloat16)
        return carry

    def hidden_step(i, carry):
        where = rows_of(i)
        gate, up = summed(0, where), summed(1, where)
        gate_sum[where, :] = gate
        up_sum[where, :] = up
        spread[0, own, where, :] = (gate * jax.nn.sigmoid(gate) * up).astype(jnp.bfloat16)
        return carry

    def factor_rows(first, count):
        def step(k, carry):
            d = row_peer(first + k // (2 * steps))
            where = rows_of(k % (2 * steps))
            gate = spread[1, d, where, :].astype(jnp.float32)
            up = spread[2, d, where, :].astype(jnp.float32)
            sigmoid_gate = jax.nn.sigmoid(gate)
            activated = gate * sigmoid_gate
            slope = sigmoid_gate * (1.0 + gate * (1.0 - sigmoid_gate))
            spread[0, d, where, :] = (activated * up).astype(jnp.bfloat16)
            factors[0, d, where, :] = up * slope
            factors[1, d, where, :] = activated
            return carry

        lax.fori_loop(0, count * 2 * steps, step, 0)

    def grad_step(i, carry):
        where = rows_of(i)
        hidden_grad = summed(2, where)
        gate, up = gate_sum[where, :], up_sum[where, :]
        sigmoid_gate = jax.nn.sigmoid(gate)
        slope = sigmoid_gate * (1.0 + gate * (1.0 - sigmoid_gate))
        spread[1, own, where, :] = (hidden_grad * up * slope).astype(jnp.bfloat16)
        spread[2, own, where, :] = (hidden_grad * (gate * sigmoid_gate)).astype(jnp.bfloat16)
        return carry

    steps = span // 16

    def hidden_rows(h):
        received(part_recv.at[pl.ds(0, 2), pl.ds(1, 2), half(h), :], pair_sem.at[h])
        lax.fori_loop(h * steps, (h + 1) * steps, hidden_step, 0)

    def grad_rows(h):
        received(part_recv.at[2, pl.ds(1, 3), half(h), :], last_part_sem.at[h])
        lax.fori_loop(h * steps, (h + 1) * steps, grad_step, 0)
        spread_grads(h)

    @pl.when(is_bottom)
    def _():
        strip = 256 if turned.shape[1] % 256 == 0 else 128

        def turn(k, inner):
            cols = pl.ds(pl.multiple_of(k * strip, strip), strip)
            for a, weight in enumerate((w_gate, w_up)):
                turned[a, cols, :] = weight[:, cols].T
            return inner

        lax.fori_loop(0, turned.shape[1] // strip, turn, 0)
        pl.semaphore_wait(go_sem.at[1], 1)
        for h in range(2):
            for a in range(2):
                via_copy(a, h).start()
        for h in range(2):
            for a in range(2):
                pair_copy(a, 1 + a, h).start()

    for a in range(2):
        relay_sum(a, 0)

    @pl.when(is_bottom)
    def _():
        for a in range(2):
            relay_sum(a, 1)
        for h in range(2):
            received(part_recv.at[pl.ds(0, 2), pl.ds(1, 2), half(h), :], pair_sem.at[h])
            lax.fori_loop(h * steps, (h + 1) * steps, sum_step, 0)
            spread_grads(h)
        relay_grads(0)

    def merge_block(c):
        @pl.when(is_top)
        def _():
            received(dy_slots.at[c, pl.ds(1, 3)], dy_recv_sem.at[c])

        @pl.when(is_bottom)
        def _():
            received(dy_slots.at[c], dy_recv_sem.at[c])

        merge(dy_slots.at[c])
        dy_whole[:, c * block:(c + 1) * block] = stage[:, :block].astype(jnp.bfloat16)

    weight_wait(2)

    for c in range(2):
        merge_block(c)

    def grad_terms_step(i, carry):
        d = section * (3 - i) + (1 - section) * i
        owner = section * row_peer(d) + (1 - section) * i
        piece = pl.ds(pl.multiple_of(owner * width, width), width)
        part_send[2, d] = lax.dot_general(
            dy_whole[...], w_down[piece, :], CONTRACT_COLS, preferred_element_type=jnp.float32
        ).astype(jnp.bfloat16)

        @pl.when(is_bottom)
        def _():
            for h in range(2):
                cross_copy(0, i, h).start()

        @pl.when(jnp.logical_and(is_top, d > 0))
        def _():
            last_part_copy(d, 0).start()

        @pl.when(jnp.logical_and(is_top, i == 1))
        def _():
            for a in range(2):
                relay_sum(a, 1)
        return carry

    lax.fori_loop(0, 4, grad_terms_step, 0)

    @pl.when(is_top)
    def _():
        for d in (3, 2, 1):
            last_part_copy(d, 1).start()
        for h in range(2):
            hidden_rows(h)
        for h in range(2):
            grad_rows(h)

    def send_branch(c):
        for d in (2, 3, 1):
            first = d * group
            branch_send[c, d] = branch[first:first + group, c * block:(c + 1) * block].astype(jnp.bfloat16)
            branch_copy(d, c).start()

    def branch_terms(d, cols):
        return lax.dot_general(
            spread[1, row_peer(d)], w_gate[cols, piece_of(d)], CONTRACT_COLS, preferred_element_type=jnp.float32
        ) + lax.dot_general(
            spread[2, row_peer(d)], w_up[cols, piece_of(d)], CONTRACT_COLS, preferred_element_type=jnp.float32
        )

    def branch_step(d, carry):
        @pl.when(d == 1)
        def _():
            relay_grads(0)
            partner_go(1)
            relay_grads(1)
            received(spread.at[2, row_peer(1)], second_sem.at[2, 0])

        @pl.when(d == 2)
        def _():
            received(spread.at[1, row_peer(2)], second_sem.at[1, 0])

        term = branch_terms(d, slice(None))

        @pl.when(d == 0)
        def _():
            branch[...] = term

        @pl.when(d > 0)
        def _():
            branch[...] += term
        return carry

    def last_branch_step(c, carry):
        @pl.when(c == 1)
        def _():
            send_branch(0)

        branch[:, block_of(c)] += branch_terms(3, block_of(c))
        return carry

    def finish_hidden():
        for h in range(2):
            second_copy(0, h, 1).wait_recv()
        received(spread.at[0, row_peer(3)], onward_sem.at[0])

    @pl.when(is_top)
    def _():
        lax.fori_loop(0, 3, branch_step, 0)
        received(spread.at[pl.ds(1, 2), row_peer(3)], onward_sem.at[1])
        lax.fori_loop(0, 2, last_branch_step, 0)

    def cross_sum(i):
        received(part_recv.at[2, i], cross_sem.at[0, i])
        total = part_send[2, i].astype(jnp.float32) + part_recv[2, i].astype(jnp.float32)
        middle[0, i] = total.astype(jnp.bfloat16)
        for h in range(2):
            cross_copy(1, i, h).start()

    def cross_grads(i):
        received(middle.at[1, i], cross_sem.at[1, i])

        def grads(k, carry):
            where = rows_of(k)
            hidden_grad = middle[0, i, where, :].astype(jnp.float32) + middle[1, i, where, :].astype(jnp.float32)
            for a in range(2):
                spread[1 + a, i, where, :] = (hidden_grad * factors[a, i, where, :]).astype(jnp.bfloat16)
            return carry

        lax.fori_loop(0, 2 * steps, grads, 0)

    def turned_terms(i, cols):
        piece = pl.ds(i * width if isinstance(i, int) else pl.multiple_of(i * width, width), width)
        term = jnp.dot(spread[1, i], turned[0, piece, cols], preferred_element_type=jnp.float32)
        return term + jnp.dot(spread[2, i], turned[1, piece, cols], preferred_element_type=jnp.float32)

    def cross_step(i, carry):
        cross_grads(i)
        term = turned_terms(i, slice(None))

        @pl.when(i == 0)
        def _():
            branch[...] = term

        @pl.when(i > 0)
        def _():
            branch[...] += term
        return carry

    def last_cross_step(c, carry):
        @pl.when(c == 1)
        def _():
            send_branch(0)

        branch[:, block_of(c)] += turned_terms(3, block_of(c))
        return carry

    @pl.when(is_bottom)
    def _():
        relay_grads(1)
        received(spread.at[2, row_peer(1)], second_sem.at[2, 0])
        received(spread.at[1, row_peer(2)], second_sem.at[1, 0])
        factor_rows(0, 3)
        for i in range(4):
            cross_sum(i)
        received(spread.at[pl.ds(1, 2), row_peer(3)], onward_sem.at[1])
        factor_rows(3, 1)
        sent(spread.at[pl.ds(1, 2), pl.ds(1, 2)], 3)
        sent(spread.at[pl.ds(1, 2), 3], 4)
        lax.fori_loop(0, 3, cross_step, 0)
        cross_grads(3)
        lax.fori_loop(0, 2, last_cross_step, 0)

    send_branch(1)

    @pl.when(is_top)
    def _():
        spread_hidden()

    @pl.when(is_bottom)
    def _():
        lax.fori_loop(0, ready.shape[0], ready_step, 0)

    for c in range(2):
        cols = slice(c * block, (c + 1) * block)
        total = dy_whole[:group, cols].astype(jnp.float32) + branch[:group, cols]
        received(branch_recv.at[c, pl.ds(1, 3)], branch_recv_sem.at[c])
        for d in (1, 2, 3):
            total = total + branch_recv[c, d].astype(jnp.float32)
        stage[:group, :block] = total
        for t in range(local):
            result[t, :, cols] = stage[t * micro:(t + 1) * micro, :block].astype(jnp.bfloat16)

        @pl.when(is_top)
        def _():
            for d in (2, 3, 1, 0):
                pass_copy(d, c).start()

    @pl.when(is_top)
    def _():
        relay_hidden()
        lax.fori_loop(0, ready.shape[0], ready_step, 0)
        finish_hidden()
        sent(dy_slots.at[:, pl.ds(1, 3)], 1)
        sent(dy_slots, 6)
        sent(part_send.at[:, pl.ds(1, 3)], 2)
        sent(spread.at[:, pl.ds(1, 2)], 3)
        sent(spread.at[:, 3], 4)

    @pl.when(is_bottom)
    def _():
        sent(part_send.at[pl.ds(0, 2), pl.ds(1, 3)], 2)
        sent(part_send.at[2], 7)
        sent(middle.at[0], 8)

    sent(branch_send.at[:, pl.ds(1, 3)], 5)
    sent(x_slots.at[pl.ds(1, 3)], 0)

def update_kernel(
    x_ref, dy_ref, packed_ref, ready_ref, grad_ref, gate_out, up_out, down_out, grad_out,
    wide_tiles, down_tiles, sem, ready_sem, grad_sem,
):
    pieces, rows, piece = packed_ref.shape[1:]
    tall = wide_tiles.shape[1]
    made, blocks = ready_ref.shape[0], x_ref.shape[1] // tall

    def where_of(j):
        return pl.ds(j * tall if isinstance(j, int) else pl.multiple_of(j * tall, tall), tall)

    ready_copies = [
        pltpu.make_async_copy(ready_ref.at[j], gate_out.at[where_of(j), :], ready_sem.at[j]) for j in range(made)
    ]
    for copy in ready_copies:
        copy.start()
    grad_copy = pltpu.make_async_copy(grad_ref, grad_out, grad_sem)
    grad_copy.start()

    def wide_step(k, carry):
        a = (k + made) // blocks
        where = where_of((k + made) % blocks)
        for p in range(pieces):
            wide_tiles[k, :, p * piece:(p + 1) * piece] = lax.dot_general(
                x_ref[:, where], packed_ref[1 + a, p], CONTRACT_ROWS, preferred_element_type=jnp.float32
            )
        for b, target in enumerate((gate_out, up_out)):
            @pl.when(a == b)
            def _():
                pltpu.make_async_copy(wide_tiles.at[k], target.at[where, :], sem.at[0]).start()
        return carry

    lax.fori_loop(0, wide_tiles.shape[0], wide_step, 0)

    def down_step(p, carry):
        where = pl.ds(pl.multiple_of(p * piece, piece), piece)
        down_tiles[p] = lax.dot_general(
            packed_ref[0, p], dy_ref[...], CONTRACT_ROWS, preferred_element_type=jnp.float32
        )
        pltpu.make_async_copy(down_tiles.at[p], down_out.at[where, :], sem.at[1]).start()
        return carry

    lax.fori_loop(0, pieces, down_step, 0)
    for copy in ready_copies:
        copy.wait()
    grad_copy.wait()
    for a, tiles in enumerate((wide_tiles, down_tiles)):
        pltpu.make_async_copy(tiles, tiles, sem.at[a]).wait()


def weight_updates(x_whole, dy_whole, packed, ready, grad):
    rows, width = x_whole.shape
    pieces, piece = packed.shape[1], packed.shape[3]
    hidden_width = pieces * piece
    made, tall = ready.shape[:2]
    f32 = jnp.float32
    vmem = pl.BlockSpec(memory_space=pltpu.VMEM)
    hbm = pl.BlockSpec(memory_space=pltpu.HBM)
    return pl.pallas_call(
        update_kernel,
        out_shape=(
            jax.ShapeDtypeStruct((width, hidden_width), f32),
            jax.ShapeDtypeStruct((width, hidden_width), f32),
            jax.ShapeDtypeStruct((hidden_width, width), f32),
            jax.ShapeDtypeStruct(grad.shape, grad.dtype),
        ),
        in_specs=[vmem] * 5,
        out_specs=(hbm,) * 4,
        scratch_shapes=[
            pltpu.VMEM((2 * width // tall - made, tall, hidden_width), f32),
            pltpu.VMEM((pieces, piece, width), f32),
            pltpu.SemaphoreType.DMA((2,)),
            pltpu.SemaphoreType.DMA((made,)),
            pltpu.SemaphoreType.DMA,
        ],
        compiler_params=pltpu.CompilerParams(vmem_limit_bytes=44 * 2**20),
        cost_estimate=pl.CostEstimate(
            flops=6 * rows * width * hidden_width,
            bytes_accessed=12 * width * hidden_width + 2 * rows * (2 * width + 3 * hidden_width),
            transcendentals=0,
        ),
    )(x_whole, dy_whole, packed, ready, grad)


def fast_shards(section_inputs, out_grad, gate_weight, up_weight, down_weight):
    panels = section_inputs[0]
    micro, local, width = panels.shape
    group = micro * local
    held = (local, micro, width)
    rows = group * lax.axis_size("col")
    hidden_width = gate_weight.shape[2]
    piece = hidden_width // lax.axis_size("row")
    hbm = pl.BlockSpec(memory_space=pltpu.HBM)
    vmem = pl.BlockSpec(memory_space=pltpu.VMEM)
    bf16, f32 = jnp.bfloat16, jnp.float32
    dma = pltpu.SemaphoreType.DMA
    block = width // 2
    tall = 256 if width % 256 == 0 else 128
    x_whole, dy_whole, packed, grad, ready = pl.pallas_call(
        relay_kernel,
        out_shape=(
            jax.ShapeDtypeStruct((rows, width), bf16),
            jax.ShapeDtypeStruct((rows, width), bf16),
            jax.ShapeDtypeStruct((3, 4, rows, piece), bf16),
            jax.ShapeDtypeStruct(held, bf16),
            jax.ShapeDtypeStruct((1, tall, hidden_width), f32),
        ),
        in_specs=[hbm] * 5,
        out_specs=(vmem,) * 5,
        scratch_shapes=[
            pltpu.VMEM((width, hidden_width), bf16),
            pltpu.VMEM((width, hidden_width), bf16),
            pltpu.VMEM((hidden_width, width), bf16),
            pltpu.VMEM((2, hidden_width, width), bf16),
            pltpu.VMEM((4, *held), bf16),
            pltpu.VMEM((2, 4, local, micro, block), bf16),
            pltpu.VMEM((rows, width), f32),
            pltpu.VMEM((3, 4, rows, piece), bf16),
            pltpu.VMEM((3, 4, rows, piece), bf16),
            pltpu.VMEM((rows, piece), f32),
            pltpu.VMEM((rows, piece), f32),
            pltpu.VMEM((2, 4, rows, piece), f32),
            pltpu.VMEM((2, 4, rows, piece), bf16),
            pltpu.VMEM((rows, width), f32),
            pltpu.VMEM((2, 4, group, block), bf16),
            pltpu.VMEM((2, 4, group, block), bf16),
            dma((3,)), dma((3,)), dma((9,)), dma((1,)), dma((2,)), dma((2, 2)), dma((2,)), dma((2,)),
            dma((3, 2)), dma((3, 2)), dma((2,)), dma((2, 4)), dma((2,)), pltpu.SemaphoreType.REGULAR((2,)),
        ],
        compiler_params=pltpu.CompilerParams(collective_id=0, has_side_effects=True, vmem_limit_bytes=46800 * 2**10),
    )(
        *(
            pltpu.with_memory_space_constraint(array, pltpu.HBM)
            for array in (
                panels.transpose(1, 0, 2), out_grad.transpose(1, 0, 2),
                gate_weight[0], up_weight[0], down_weight[0],
            )
        )
    )
    *grads, grad = weight_updates(x_whole, dy_whole, packed, ready, grad)
    grad = grad.transpose(1, 0, 2)
    return (grad[None], *(g[None] for g in grads))


def fits_kernel(mesh, gate_weight, section_inputs):
    sizes = mesh.shape
    if (sizes["section"], sizes["row"], sizes["col"]) != (2, 4, 4):
        return False
    piece = gate_weight.shape[2] // (sizes["row"] * sizes["col"])
    local = section_inputs.shape[1] * section_inputs.shape[2] // sizes["col"]
    return piece % 128 == 0 and section_inputs.shape[3] % (256 * sizes["row"]) == 0 and local % 8 == 0 and (local * sizes["col"]) % 32 == 0


def solution(mesh):
    specs = dict(
        mesh=mesh,
        in_specs=(
            P("section", None, "col", "row"),
            P(None, "col", "row"),
            P("section", "row", "col"),
            P("section", "row", "col"),
            P("section", "col", "row"),
        ),
        out_specs=(
            P("section", None, "col", "row"),
            P("section", "row", "col"),
            P("section", "row", "col"),
            P("section", "col", "row"),
        ),
        check_vma=False,
    )

    def run(section_inputs, out_grad, gate_weight, up_weight, down_weight):
        body = fast_shards if fits_kernel(mesh, gate_weight, section_inputs) else shards
        return jax.shard_map(body, **specs)(section_inputs, out_grad, gate_weight, up_weight, down_weight)

    return run
```
